32 devices in a mesh: seq: 8 (over y, x, core), stretch: 4 (over z).
Axes of the slice: x: 2, y: 2, z: 4, core: 2. Of those that a mesh axis runs over, the one named last changes fastest.
Arguments:
- queries: bfloat16 [4096, 1792], P(('stretch', 'seq')), may hold values from -140 to 140
- keys: bfloat16 [4096, 256], P(('stretch', 'seq')), may hold values from -6 to 6
- values: bfloat16 [4096, 256], P(('stretch', 'seq')), may hold values from -6 to 6
Outputs:
- attended: bfloat16 [4096, 1792], P(('stretch', 'seq'))
The draws below stay inside these ranges and needn't reach their ends.
All inputs are finite; a program needn't handle non-finite values.
Results may differ from the reference program's by a relative error of at most 0.011.
Values may be sent and summed in bfloat16 or wider, within the bound.
A program may use at most 64 MiB of HBM per device.

```python
import math
import jax
import jax.numpy as jnp
from jax import lax

QUERY_HEADS = 14
KEY_VALUE_HEADS = 2
HEAD_SIZE = 128
BLOCKS = 4
BLOCK_TOKENS = 1024
SEQS = 1
TOTAL_TOKENS = 4096


def base_keys(key):
    return jnp.clip(jax.random.normal(jax.random.fold_in(key, 11), (TOTAL_TOKENS, KEY_VALUE_HEADS * HEAD_SIZE), jnp.float32), -6.0, 6.0)


def draw_keys(key, part):
    rotary_base = base_keys(key)
    return rotary_base.astype(jnp.bfloat16)


def draw_queries(key, part):
    noise = 3.0 * jnp.clip(jax.random.normal(jax.random.fold_in(key, 17), (TOTAL_TOKENS, QUERY_HEADS * HEAD_SIZE), jnp.float32), -6.0, 6.0)
    return noise.astype(jnp.bfloat16)


def steps_of(key, dims, cuts, low, largest):
    gain = 1.0
    for position, parts in cuts:
        steps = jax.random.uniform(jax.random.fold_in(jax.random.fold_in(key, 6), position), (parts,), jnp.float32, low / len(cuts), largest / len(cuts))
        gain = gain * jnp.repeat(jnp.exp(steps), dims[position] // parts).reshape((-1,) + (1,) * (len(dims) - 1 - position))
    return gain


def bell_draw(stream_key, extent, width, most, cuts=(), kind=jnp.bfloat16):
    level = steps_of(stream_key, extent, cuts, -0.22, 0.18) if cuts else 1.0
    values = jax.random.normal(stream_key, extent, jnp.float32) * width * level
    return jnp.minimum(jnp.maximum(values, -most), most).astype(kind)


def setup_inputs(seed: int = 0) -> dict:
    key_of = jax.random.split(jax.random.key(seed), 4)
    return {
        "queries": draw_queries(jax.random.fold_in(key_of[3], 71), 0),
        "keys": draw_keys(jax.random.fold_in(key_of[3], 71), 0),
        "values": bell_draw(key_of[2], (TOTAL_TOKENS, KEY_VALUE_HEADS * HEAD_SIZE), 1.0, 6.0, ((0, 32),)),
    }


def apply_rotary(rows, token_positions, heads):
    half_width = HEAD_SIZE // 2
    inverse = 10000000.0 ** (-(jnp.arange(half_width, dtype=jnp.float32) * 2.0) / HEAD_SIZE)
    angles = token_positions.astype(jnp.float32)[:, None] * inverse[None, :]
    cosine = jnp.cos(angles)[:, None, :]
    sine_part = jnp.sin(angles)[:, None, :]
    shaped = rows.reshape(rows.shape[0], heads, HEAD_SIZE).astype(jnp.float32)
    first_half = shaped[..., :half_width]
    second_half = shaped[..., half_width:]
    turned = jnp.concatenate([first_half * cosine - second_half * sine_part, second_half * cosine + first_half * sine_part], axis=-1)
    return turned.reshape(rows.shape[0], heads * HEAD_SIZE).astype(jnp.bfloat16)

def reference(queries, keys, values):
    head_cluster = QUERY_HEADS // KEY_VALUE_HEADS
    score_scale = 1.0 / math.sqrt(HEAD_SIZE)
    rows_of_block = min(256, BLOCK_TOKENS)
    inner_position = jnp.arange(BLOCK_TOKENS, dtype=jnp.int32)
    outputs = [None] * (SEQS * BLOCKS)
    for sequence in range(SEQS):
        for block_position in range(BLOCKS):
            leading_row = (block_position * SEQS + sequence) * BLOCK_TOKENS
            query_rows = queries[leading_row:leading_row + BLOCK_TOKENS]
            rotated_sets = {'near': apply_rotary(query_rows, inner_position, QUERY_HEADS), 'next': apply_rotary(query_rows, inner_position + BLOCK_TOKENS, QUERY_HEADS), 'far': apply_rotary(query_rows, jnp.full((BLOCK_TOKENS,), 2 * BLOCK_TOKENS - 1, jnp.int32), QUERY_HEADS)}
            key_list = []
            value_list = []
            for source in range(block_position + 1):
                source_row = (source * SEQS + sequence) * BLOCK_TOKENS
                key_list.append(apply_rotary(keys[source_row:source_row + BLOCK_TOKENS], inner_position, KEY_VALUE_HEADS))
                value_list.append(values[source_row:source_row + BLOCK_TOKENS])
            rotated_keys = jnp.concatenate(key_list, axis=0).astype(jnp.float32).reshape(-1, KEY_VALUE_HEADS, HEAD_SIZE)
            rows_of_values = jnp.concatenate(value_list, axis=0).astype(jnp.float32).reshape(-1, KEY_VALUE_HEADS, HEAD_SIZE)

            def one_block(block_number, block_position=block_position, rotated_sets=rotated_sets, rotated_keys=rotated_keys, rows_of_values=rows_of_values):
                row_start = block_number * rows_of_block
                pieces = []
                for source in range(block_position + 1):
                    chosen = 'near' if source == block_position else 'next' if source == block_position - 1 else 'far'
                    block_of_query = lax.dynamic_slice_in_dim(rotated_sets[chosen], row_start, rows_of_block, 0)
                    block_of_query = block_of_query.astype(jnp.float32).reshape(rows_of_block, KEY_VALUE_HEADS, head_cluster, HEAD_SIZE)
                    key_block = rotated_keys[source * BLOCK_TOKENS:(source + 1) * BLOCK_TOKENS]
                    scores = jnp.einsum('rkgd,skd->kgrs', block_of_query, key_block, precision=lax.Precision.HIGHEST) * score_scale
                    if source == block_position:
                        allowed = (row_start + jnp.arange(rows_of_block, dtype=jnp.int32))[:, None] >= jnp.arange(BLOCK_TOKENS, dtype=jnp.int32)[None, :]
                        scores = jnp.where(allowed, scores, -1e+30)
                    pieces.append(scores)
                scores = jnp.concatenate(pieces, axis=-1)
                row_max = lax.optimization_barrier(jnp.max(scores, axis=-1, keepdims=True))
                weights = jnp.exp(scores - row_max)
                row_sum = lax.optimization_barrier(jnp.sum(weights, axis=-1))
                attended = jnp.einsum('kgrs,skd->rkgd', weights, rows_of_values, precision=lax.Precision.HIGHEST)
                attended = attended / jnp.transpose(row_sum, (2, 0, 1))[..., None]
                return attended.reshape(rows_of_block, QUERY_HEADS * HEAD_SIZE).astype(jnp.bfloat16)
            result = lax.map(one_block, jnp.arange(BLOCK_TOKENS // rows_of_block, dtype=jnp.int32))
            outputs[block_position * SEQS + sequence] = result.reshape(BLOCK_TOKENS, QUERY_HEADS * HEAD_SIZE)
    return jnp.concatenate(outputs, axis=0)
```

```python
import functools
import math

import jax
import jax.numpy as jnp
import numpy as np
from jax import lax
from jax.experimental import pallas as pl
from jax.experimental.pallas import tpu as pltpu
from jax.sharding import PartitionSpec as P

QUERY_HEADS = 14
KEY_VALUE_HEADS = 2
HEAD_SIZE = 128
BLOCKS = 4
CLUSTER = QUERY_HEADS // KEY_VALUE_HEADS
WIDTH = CLUSTER * HEAD_SIZE
HALF = HEAD_SIZE // 2
SCALE = math.log2(math.e) / math.sqrt(HEAD_SIZE)
MASKED = -1e30


def rotary_table(positions):
    inverse = 10000000.0 ** (-(np.arange(HALF, dtype=np.float64) * 2.0) / HEAD_SIZE)
    angles = np.arange(positions, dtype=np.float64)[:, None] * inverse[None, :]
    return np.concatenate([np.cos(angles), np.sin(angles)], axis=1).astype(np.float32)


def turned_rows(rows, table):
    swapped = pltpu.roll(table, HALF, 1)
    low = lax.broadcasted_iota(jnp.int32, table.shape, 1) < HALF
    cosine, sine = jnp.where(low, table, swapped), jnp.where(low, -swapped, table)
    x = rows.astype(jnp.float32)
    return (x * cosine + pltpu.roll(x, HALF, 1) * sine).astype(jnp.bfloat16)


def turned_columns(columns, table):
    x, y = columns[:HALF], columns[HALF:]
    cosine, sine = table[:HALF], table[HALF:]
    return jnp.concatenate([x * cosine - y * sine, y * cosine + x * sine], axis=0).astype(
        jnp.bfloat16
    )


def kernel(
    shape, q_in, k_in, v_in, rows_in, columns_in, far_in, out,
    q_own, q_swap, k_own, v_own, k_send, v_send, k_buf, v_buf, q_rot,
    s_even, s_odd, w_even, w_odd, row_table, near_table, next_table, far_table,
    peak, total, fade, top, acc, o_buf,
    local_sem, swap_send, swap_recv, slot_recv, first_send, flat_send, relay_send, lift_send,
    out_local, out_send, out_recv,
):
    shard, pairs, side_a, side_b, sequences, span = shape
    rows = 2 * shard
    length = pairs * rows
    s = lax.axis_index("seq")
    g = lax.axis_index("stretch")
    h = s % 2
    p = s // 2
    a = p // side_b
    b = p % side_b
    n = g // sequences
    last = BLOCKS - 1
    partner = {"seq": s + 1 - 2 * h}
    mesh_type = pl.DeviceIdType.MESH

    def pair_at(a_index, b_index):
        return a_index * side_b + b_index

    def device_at(pair, core):
        return {"seq": 2 * pair + core}

    def block_at(shift, core):
        return {"seq": 2 * p + core, "stretch": g + shift * sequences}

    a_peers = [pair_at((a + i) % side_a, b) for i in range(1, side_a)]
    b_peers = [pair_at(a, (b + j) % side_b) for j in range(1, side_b)]
    diagonal = [
        pair_at((a + i) % side_a, (b + j) % side_b)
        for i in range(1, side_a)
        for j in range(1, side_b)
    ]

    def at(start, size, unit):
        return pl.ds(pl.multiple_of(start, unit), size)

    def head_columns(head):
        return at(head * HEAD_SIZE, HEAD_SIZE, HEAD_SIZE)

    def own_columns(core):
        return at(core * WIDTH, WIDTH, HEAD_SIZE)

    def half_columns(core):
        return at(core * shard, shard, shard)

    mine = half_columns(h)
    theirs = half_columns(1 - h)

    local = [
        (k_in, k_own),
        (rows_in.at[at(p * rows + h * shard, shard, shard), :], row_table),
        (v_in, v_own),
        (q_in, q_own),
        (columns_in.at[:, at(p * rows, rows, rows)], near_table),
        (columns_in.at[:, at(length + p * rows, rows, rows)], next_table),
        (far_in, far_table),
    ]
    local = [
        pltpu.make_async_copy(src, dst, local_sem.at[i]) for i, (src, dst) in enumerate(local)
    ]
    for copy in local:
        copy.start()

    barrier = pltpu.get_barrier_semaphore()

    def greet(device):
        pl.semaphore_signal(barrier, inc=1, device_id=device, device_id_type=mesh_type)

    for core in range(2):
        @pl.when(n < last)
        def _():
            greet(block_at(1, core))

        @pl.when(n > 0)
        def _():
            greet(block_at(-1, core))

        @pl.when(n == 0)
        def _():
            greet(block_at(last, core))

        @pl.when(n == last)
        def _():
            greet(block_at(-last, core))

        for peer in a_peers + b_peers:
            greet(device_at(peer, core))
    greet(partner)

    def rotate_queries(source, half):
        near, later, far = near_table[:, half], next_table[:, half], far_table[:, :1]
        for c in range(CLUSTER):
            x = source(c).T.astype(jnp.float32)
            q_rot[0, c, :, half] = turned_columns(x, near)
            q_rot[1, c, :, half] = turned_columns(x, later)
            q_rot[2, c, :, half] = turned_columns(x, far)

    local[0].wait()
    local[1].wait()
    local[2].wait()
    for head in range(KEY_VALUE_HEADS):
        columns = slice(head * HEAD_SIZE, (head + 1) * HEAD_SIZE)
        k_send[head] = turned_rows(k_own[:, columns], row_table[...])
        v_send[head] = v_own[:, columns].T
    k_buf[0, at(p * rows + h * shard, shard, shard), :] = k_send[h]
    v_buf[0, p, h] = v_send[h]
    for copy in local[3:]:
        copy.wait()
    rotate_queries(lambda c: q_own[:, at(h * WIDTH + c * HEAD_SIZE, HEAD_SIZE, HEAD_SIZE)], mine)

    pl.semaphore_wait(barrier, 1 + 2 * (len(a_peers) + len(b_peers)) + 4)

    def slot(t, d, pair):
        if t == 0:
            return k_buf.at[d, at(pair * rows, rows, rows), :]
        return v_buf.at[d, pair]

    def part(t, d, pair, core):
        if t == 0:
            return k_buf.at[d, at(pair * rows + core * shard, shard, shard), :]
        return v_buf.at[d, pair, core]

    def message(t, d, pair, device, d_to, send_sem):
        return pltpu.make_async_remote_copy(
            src_ref=slot(t, d, pair), dst_ref=slot(t, d_to, pair),
            send_sem=send_sem, recv_sem=slot_recv.at[t, d_to, pair],
            device_id=device, device_id_type=mesh_type,
        )

    def first(t, core, device, d_to, i):
        return pltpu.make_async_remote_copy(
            src_ref=(k_send, v_send)[t].at[core], dst_ref=part(t, d_to, p, h),
            send_sem=first_send.at[t, core, i], recv_sem=slot_recv.at[t, d_to, p],
            device_id=device, device_id_type=mesh_type,
        )

    def arrived(t, d, pair):
        message(t, d, pair, partner, d, lift_send.at[0, 0, 0, 0]).wait_recv()

    def routes(t, d):
        if d == 0:
            found = [(n < last, 1, 1), (n == 0, last, last)]
            return found + [(n == 1, -1, last)] if t == 1 else found
        if d == 1:
            return [((n == 1) if t == 1 else (n == 1) | (n == 2), 1, 2)]
        return [(n == 0, last, 2)] if d == last and t == 1 else []

    def firsts(t):
        peers = a_peers + b_peers
        plain = [
            first(t, core, device_at(peer, core), 0, i)
            for i, peer in enumerate(peers)
            for core in range(2)
        ]
        lifted = [
            (when, first(t, core, block_at(shift, core), d_to, len(peers) + i))
            for i, (when, shift, d_to) in enumerate(routes(t, 0))
            for core in range(2)
        ]
        own = pltpu.make_async_remote_copy(
            src_ref=(k_send, v_send)[t].at[1 - h], dst_ref=part(t, 0, p, h),
            send_sem=swap_send.at[t], recv_sem=swap_recv.at[t],
            device_id=partner, device_id_type=mesh_type,
        )
        return own, plain, lifted

    query_swap = pltpu.make_async_remote_copy(
        src_ref=q_own.at[:, own_columns(1 - h)], dst_ref=q_swap,
        send_sem=swap_send.at[2], recv_sem=swap_recv.at[2],
        device_id=partner, device_id_type=mesh_type,
    )

    for t in range(2):
        own, plain, lifted = firsts(t)
        for copy in plain:
            copy.start()
        for when, copy in lifted:
            pl.when(when)(copy.start)
        own.start()
    query_swap.start()

    def flat(t, d):
        return [
            message(t, d, p, device_at(peer, h), d, flat_send.at[t, d, i])
            for i, peer in enumerate(b_peers + a_peers)
        ]

    def relays(t):
        sources, targets = (b_peers, a_peers) if t == 0 else (a_peers, b_peers)
        return [
            [
                message(t, 0, source, device_at(target, h), 0, relay_send.at[t, i, j])
                for j, target in enumerate(targets)
            ]
            for i, source in enumerate(sources)
        ]

    def lifts(t, d, pair, i):
        return [
            (when, message(t, d, pair, block_at(shift, h), d_to, lift_send.at[t, d, i, k]))
            for k, (when, shift, d_to) in enumerate(routes(t, d))
        ]

    def lift(t, d, pair, i):
        for when, copy in lifts(t, d, pair, i):
            pl.when(when)(copy.start)

    def column(t, d):
        arrived(t, d, p)
        for copy in flat(t, d):
            copy.start()
        lift(t, d, p, 0)

    def scores(c, d, line, version, causal, into, side):
        found = jnp.dot(
            k_buf[d, at(line * span, span, span), :], q_rot[version, c],
            preferred_element_type=jnp.float32,
        )
        if causal:
            key = lax.broadcasted_iota(jnp.int32, found.shape, 0)
            row = b * rows + lax.broadcasted_iota(jnp.int32, found.shape, 1)
            found = jnp.where(row >= key, found, MASKED)
        into[...] = found
        top[side] = jnp.max(found.reshape(span // 8, 8, rows), axis=0)

    def weigh(c, causal, source, into, side):
        new = jnp.max(top[side], axis=0, keepdims=True) * SCALE
        if causal:
            new = jnp.broadcast_to(new, (8, rows))
        else:
            old = peak[c]
            new = jnp.maximum(old, new)
            fade[side] = jnp.exp2(old - new)
        peak[c] = new
        new = new[:1]
        added = None
        for start in range(0, span, 64):
            weights = jnp.exp2(source[start : start + 64, :] * SCALE - new)
            some = jnp.sum(weights.reshape(8, 8, rows), axis=0)
            added = some if added is None else added + some
            into[start : start + 64, :] = weights.astype(jnp.bfloat16)
        total[c] = added if causal else total[c] * fade[side] + added

    def gather(c, d, line, causal, source, side):
        values = jnp.concatenate(
            [v_buf[d, line * side_b + i // 2, i % 2] for i in range(2 * side_b)], axis=1
        )
        product = jnp.dot(values, source[...], preferred_element_type=jnp.float32)
        acc[c] = product if causal else acc[c] * fade[side][:1] + product

    def attend(d, line, causal):
        version = jnp.minimum(d, 2)
        s_buf, w_buf = (s_even, s_odd), (w_even, w_odd)
        scores(0, d, line, version, causal, s_buf[0], 0)
        for c in range(CLUSTER):
            if c + 1 < CLUSTER:
                scores(c + 1, d, line, version, causal, s_buf[(c + 1) % 2], (c + 1) % 2)
            if c > 0:
                gather(c - 1, d, line, causal, w_buf[(c - 1) % 2], (c - 1) % 2)
            weigh(c, causal, s_buf[c % 2], w_buf[c % 2], c % 2)
        gather(CLUSTER - 1, d, line, causal, w_buf[(CLUSTER - 1) % 2], (CLUSTER - 1) % 2)

    query_swap.wait_recv()
    rotate_queries(lambda c: q_swap[:, c * HEAD_SIZE : (c + 1) * HEAD_SIZE], theirs)
    for t in range(2):
        pltpu.make_async_remote_copy(
            src_ref=(k_send, v_send)[t].at[h], dst_ref=part(t, 0, p, 1 - h),
            send_sem=swap_send.at[t], recv_sem=swap_recv.at[t],
            device_id=partner, device_id_type=mesh_type,
        ).wait_recv()

    for t, sources in ((0, b_peers), (1, a_peers)):
        for source, copies in zip(sources, relays(t)):
            arrived(t, 0, source)
            for copy in copies:
                copy.start()

        @pl.when(n > 0)
        def _():
            column(t, 1)

        @pl.when(n == last)
        def _():
            column(t, last)

    @pl.when(n == 0)
    def _():
        arrived(1, last, p)
        lift(1, last, p, 0)

    for source in b_peers:
        arrived(1, 0, source)
    attend(0, a, True)

    def visit(j, carry):
        i = j % side_a
        place = j // side_a
        d = jnp.where(place < 2, place, jnp.where((n == last) & (place == 2), last, 2))
        line = (a + i) % side_a

        for t in range(2):
            @pl.when((j == 1 + t) & (n >= 2))
            def _():
                column(t, 2)

        for t in range(2):
            @pl.when(i == 0)
            def _():
                for source in b_peers:
                    arrived(t, d, source)

            for shift in range(1, side_a):
                @pl.when(i == shift)
                def _():
                    there = (a + shift) % side_a

                    @pl.when((t == 0) | (d > 0))
                    def _():
                        arrived(t, d, pair_at(there, b))

                    for k in range(1, side_b):
                        pair = pair_at(there, (b + k) % side_b)
                        arrived(t, d, pair)
                        for level in range(2):
                            @pl.when(d == level)
                            def _():
                                lift(t, level, pair, 1 + (shift - 1) * (side_b - 1) + k - 1)

        @pl.when((d > 0) | (line < a))
        def _():
            attend(d, line, False)

        return carry

    lax.fori_loop(1, side_a * (n + 1), visit, 0)

    @pl.when(n == 0)
    def _():
        for i, pair in enumerate(diagonal):
            arrived(1, last, pair)
            lift(1, last, pair, 1 + i)

    def results(c):
        where = head_columns(h * CLUSTER + c)
        return (
            pltpu.make_async_copy(o_buf.at[c, mine, :], out.at[:, where], out_local.at[c]),
            pltpu.make_async_remote_copy(
                src_ref=o_buf.at[c, theirs, :], dst_ref=out.at[:, where],
                send_sem=out_send.at[c], recv_sem=out_recv.at[c],
                device_id=partner, device_id_type=mesh_type,
            ),
        )

    for c in range(CLUSTER + 1):
        if c < CLUSTER:
            share = 1.0 / jnp.sum(total[c], axis=0, keepdims=True)
            o_buf[c] = (acc[c] * share).astype(jnp.bfloat16).T
        if c > 0:
            for copy in results(c - 1):
                copy.start()

    query_swap.wait_send()
    for t in range(2):
        own, plain, lifted = firsts(t)
        own.wait_send()
        for copy in plain:
            copy.wait_send()
        for when, copy in lifted:
            pl.when(when)(copy.wait_send)
        for copies in relays(t):
            for copy in copies:
                copy.wait_send()

    for t in range(2):
        for d in range(1, BLOCKS):
            @pl.when(d <= n)
            def _():
                for copy in flat(t, d):
                    copy.wait_send()
        for d in range(BLOCKS):
            for i, pair in enumerate([p] + diagonal):
                if d > 0 or i > 0:
                    for when, copy in lifts(t, d, pair, i):
                        pl.when(when)(copy.wait_send)

    for c in range(CLUSTER):
        here, there = results(c)
        here.wait()
        there.wait_send()
        there.wait_recv()


def on_device(queries, keys, values):
    shard = queries.shape[0]
    pairs = lax.axis_size("seq") // 2
    sequences = lax.axis_size("stretch") // BLOCKS
    side_a = max(i for i in range(1, pairs + 1) if pairs % i == 0 and i * i <= pairs)
    side_b = pairs // side_a
    rows = 2 * shard
    length = pairs * rows
    span = side_b * rows
    shape = (shard, pairs, side_a, side_b, sequences, span)
    table = rotary_table(2 * length)
    far = np.broadcast_to(table[-1][:, None], (HEAD_SIZE, HEAD_SIZE))
    dma = pltpu.SemaphoreType.DMA
    peers = max(side_a - 1 + side_b - 1, 1)
    most = max(side_b - 1, side_a - 1, 1)
    lifted = 1 + (side_a - 1) * (side_b - 1)
    bf16, f32 = jnp.bfloat16, jnp.float32
    return pl.pallas_call(
        functools.partial(kernel, shape),
        out_shape=jax.ShapeDtypeStruct(queries.shape, bf16),
        in_specs=[pl.BlockSpec(memory_space=pl.ANY)] * 6,
        out_specs=pl.BlockSpec(memory_space=pl.ANY),
        scratch_shapes=[
            pltpu.VMEM((shard, 2 * WIDTH), bf16),
            pltpu.VMEM((shard, WIDTH), bf16),
            pltpu.VMEM((shard, 2 * HEAD_SIZE), bf16),
            pltpu.VMEM((shard, 2 * HEAD_SIZE), bf16),
            pltpu.VMEM((2, shard, HEAD_SIZE), bf16),
            pltpu.VMEM((2, HEAD_SIZE, shard), bf16),
            pltpu.VMEM((BLOCKS, length, HEAD_SIZE), bf16),
            pltpu.VMEM((BLOCKS, pairs, 2, HEAD_SIZE, shard), bf16),
            pltpu.VMEM((3, CLUSTER, HEAD_SIZE, rows), bf16),
            pltpu.VMEM((span, rows), f32),
            pltpu.VMEM((span, rows), f32),
            pltpu.VMEM((span, rows), bf16),
            pltpu.VMEM((span, rows), bf16),
            pltpu.VMEM((shard, HEAD_SIZE), f32),
            pltpu.VMEM((HEAD_SIZE, rows), f32),
            pltpu.VMEM((HEAD_SIZE, rows), f32),
            pltpu.VMEM((HEAD_SIZE, HEAD_SIZE), f32),
            pltpu.VMEM((CLUSTER, 8, rows), f32),
            pltpu.VMEM((CLUSTER, 8, rows), f32),
            pltpu.VMEM((2, 8, rows), f32),
            pltpu.VMEM((2, 8, rows), f32),
            pltpu.VMEM((CLUSTER, HEAD_SIZE, rows), f32),
            pltpu.VMEM((CLUSTER, rows, HEAD_SIZE), bf16),
            dma((7,)),
            dma((3,)),
            dma((3,)),
            dma((2, BLOCKS, pairs)),
            dma((2, 2, peers + 3)),
            dma((2, BLOCKS, peers)),
            dma((2, most, most)),
            dma((2, BLOCKS, lifted, 3)),
            dma((CLUSTER,)),
            dma((CLUSTER,)),
            dma((CLUSTER,)),
        ],
        compiler_params=pltpu.CompilerParams(
            collective_id=0, has_side_effects=True, vmem_limit_bytes=60 * 1024 * 1024
        ),
    )(
        queries, keys, values,
        jnp.asarray(table[:length]), jnp.asarray(np.ascontiguousarray(table.T)), jnp.asarray(far),
    )


def solution(mesh):
    placed = P(("stretch", "seq"), None)
    return jax.shard_map(
        on_device, mesh=mesh, in_specs=(placed,) * 3, out_specs=placed, check_vma=False
    )
```

```python
import functools
import math

import jax
import jax.numpy as jnp
import numpy as np
from jax import lax
from jax.experimental import pallas as pl
from jax.experimental.pallas import tpu as pltpu
from jax.sharding import PartitionSpec as P

QUERY_HEADS = 14
KEY_VALUE_HEADS = 2
HEAD_SIZE = 128
BLOCKS = 4
CLUSTER = QUERY_HEADS // KEY_VALUE_HEADS
WIDTH = CLUSTER * HEAD_SIZE
HALF = HEAD_SIZE // 2
SCALE = math.log2(math.e) / math.sqrt(HEAD_SIZE)
MASKED = -1e30


def rotary_table(positions):
    inverse = 10000000.0 ** (-(np.arange(HALF, dtype=np.float64) * 2.0) / HEAD_SIZE)
    angles = np.arange(positions, dtype=np.float64)[:, None] * inverse[None, :]
    return np.concatenate([np.cos(angles), np.sin(angles)], axis=1).astype(np.float32)


def turned_rows(rows, table):
    swapped = pltpu.roll(table, HALF, 1)
    low = lax.broadcasted_iota(jnp.int32, table.shape, 1) < HALF
    cosine, sine = jnp.where(low, table, swapped), jnp.where(low, -swapped, table)
    x = rows.astype(jnp.float32)
    return (x * cosine + pltpu.roll(x, HALF, 1) * sine).astype(jnp.bfloat16)


def turned_columns(columns, table):
    x, y = columns[:HALF], columns[HALF:]
    cosine, sine = table[:HALF], table[HALF:]
    return jnp.concatenate([x * cosine - y * sine, y * cosine + x * sine], axis=0).astype(
        jnp.bfloat16
    )


def kernel(
    shape, q_in, k_in, v_in, rows_in, columns_in, far_in, out,
    q_own, q_swap, k_own, v_own, k_send, v_send, k_buf, v_buf, q_rot,
    s_even, s_odd, w_even, w_odd, row_table, near_table, next_table, far_table,
    peak, total, fade, top, acc, o_buf,
    local_sem, swap_send, swap_recv, slot_recv, first_send, flat_send, relay_send, lift_send,
    out_local, out_send, out_recv,
):
    shard, pairs, side_a, side_b, sequences, span = shape
    rows = 2 * shard
    length = pairs * rows
    s = lax.axis_index("seq")
    g = lax.axis_index("stretch")
    h = s % 2
    p = s // 2
    a = p // side_b
    b = p % side_b
    n = g // sequences
    last = BLOCKS - 1
    partner = {"seq": s + 1 - 2 * h}
    mesh_type = pl.DeviceIdType.MESH

    def pair_at(a_index, b_index):
        return a_index * side_b + b_index

    def device_at(pair, core):
        return {"seq": 2 * pair + core}

    def block_at(shift, core):
        return {"seq": 2 * p + core, "stretch": g + shift * sequences}

    a_peers = [pair_at((a + i) % side_a, b) for i in range(1, side_a)]
    b_peers = [pair_at(a, (b + j) % side_b) for j in range(1, side_b)]
    diagonal = [
        pair_at((a + i) % side_a, (b + j) % side_b)
        for i in range(1, side_a)
        for j in range(1, side_b)
    ]

    def at(start, size, unit):
        return pl.ds(pl.multiple_of(start, unit), size)

    def head_columns(head):
        return at(head * HEAD_SIZE, HEAD_SIZE, HEAD_SIZE)

    def own_columns(core):
        return at(core * WIDTH, WIDTH, HEAD_SIZE)

    def half_columns(core):
        return at(core * shard, shard, shard)

    mine = half_columns(h)
    theirs = half_columns(1 - h)

    local = [
        (k_in, k_own),
        (rows_in.at[at(p * rows + h * shard, shard, shard), :], row_table),
        (v_in, v_own),
        (q_in, q_own),
        (columns_in.at[:, at(p * rows, rows, rows)], near_table),
        (columns_in.at[:, at(length + p * rows, rows, rows)], next_table),
        (far_in, far_table),
    ]
    local = [
        pltpu.make_async_copy(src, dst, local_sem.at[i]) for i, (src, dst) in enumerate(local)
    ]
    for copy in local:
        copy.start()

    barrier = pltpu.get_barrier_semaphore()

    def greet(device):
        pl.semaphore_signal(barrier, inc=1, device_id=device, device_id_type=mesh_type)

    for core in range(2):
        @pl.when(n < last)
        def _():
            greet(block_at(1, core))

        @pl.when(n > 0)
        def _():
            greet(block_at(-1, core))

        @pl.when(n == 0)
        def _():
            greet(block_at(last, core))

        @pl.when(n == last)
        def _():
            greet(block_at(-last, core))

        for peer in a_peers + b_peers:
            greet(device_at(peer, core))
    greet(partner)

    def rotate_queries(source, half):
        near, later, far = near_table[:, half], next_table[:, half], far_table[:, :1]
        for c in range(CLUSTER):
            x = source(c).T.astype(jnp.float32)
            q_rot[0, c, :, half] = turned_columns(x, near)
            q_rot[1, c, :, half] = turned_columns(x, later)
            q_rot[2, c, :, half] = turned_columns(x, far)

    local[0].wait()
    local[1].wait()
    local[2].wait()
    for head in range(KEY_VALUE_HEADS):
        columns = slice(head * HEAD_SIZE, (head + 1) * HEAD_SIZE)
        k_send[head] = turned_rows(k_own[:, columns], row_table[...])
        v_send[head] = v_own[:, columns].T
    k_buf[0, at(p * rows + h * shard, shard, shard), :] = k_send[h]
    v_buf[0, p, h] = v_send[h]
    for copy in local[3:]:
        copy.wait()
    rotate_queries(lambda c: q_own[:, at(h * WIDTH + c * HEAD_SIZE, HEAD_SIZE, HEAD_SIZE)], mine)

    pl.semaphore_wait(barrier, 1 + 2 * (len(a_peers) + len(b_peers)) + 4)

    def slot(t, d, pair):
        if t == 0:
            return k_buf.at[d, at(pair * rows, rows, rows), :]
        return v_buf.at[d, pair]

    def part(t, d, pair, core):
        if t == 0:
            return k_buf.at[d, at(pair * rows + core * shard, shard, shard), :]
        return v_buf.at[d, pair, core]

    def message(t, d, pair, device, d_to, send_sem):
        return pltpu.make_async_remote_copy(
            src_ref=slot(t, d, pair), dst_ref=slot(t, d_to, pair),
            send_sem=send_sem, recv_sem=slot_recv.at[t, d_to, pair],
            device_id=device, device_id_type=mesh_type,
        )

    def first(t, core, device, d_to, i):
        return pltpu.make_async_remote_copy(
            src_ref=(k_send, v_send)[t].at[core], dst_ref=part(t, d_to, p, h),
            send_sem=first_send.at[t, core, i], recv_sem=slot_recv.at[t, d_to, p],
            device_id=device, device_id_type=mesh_type,
        )

    def arrived(t, d, pair):
        message(t, d, pair, partner, d, lift_send.at[0, 0, 0, 0]).wait_recv()

    def column_routes(d):
        if d == 0:
            return [(n < last, 1, 1), (n == 0, last, last)]
        return [((n > 0) & (n < last), 1, 2)] if d == 1 else []

    def diagonal_routes(d):
        return [(n == last - 1, 1, 1), (n == 0, last, last)] if d == 0 else []

    def firsts(t):
        peers = a_peers + b_peers
        plain = [
            first(t, core, device_at(peer, core), 0, i)
            for i, peer in enumerate(peers)
            for core in range(2)
        ]
        lifted = [
            (when, first(t, core, block_at(shift, core), d_to, len(peers) + i))
            for i, (when, shift, d_to) in enumerate(column_routes(0))
            for core in range(2)
        ]
        own = pltpu.make_async_remote_copy(
            src_ref=(k_send, v_send)[t].at[1 - h], dst_ref=part(t, 0, p, h),
            send_sem=swap_send.at[t], recv_sem=swap_recv.at[t],
            device_id=partner, device_id_type=mesh_type,
        )
        return own, plain, lifted

    query_swap = pltpu.make_async_remote_copy(
        src_ref=q_own.at[:, own_columns(1 - h)], dst_ref=q_swap,
        send_sem=swap_send.at[2], recv_sem=swap_recv.at[2],
        device_id=partner, device_id_type=mesh_type,
    )

    for t in range(2):
        own, plain, lifted = firsts(t)
        for copy in plain:
            copy.start()
        for when, copy in lifted:
            pl.when(when)(copy.start)
        own.start()
    query_swap.start()

    def flat(t, d):
        return [
            message(t, d, p, device_at(peer, h), d, flat_send.at[t, d, i])
            for i, peer in enumerate(b_peers + a_peers)
        ]

    def relayed(d):
        return (d == 0) | (n < last) | (d == 2)

    def relay(t, d, i, source):
        return [
            message(t, d, source, device_at(target, h), d, relay_send.at[t, d, i, j])
            for j, target in enumerate((a_peers, b_peers)[t])
        ]

    def pass_on(t, d):
        for i, source in enumerate((b_peers, a_peers)[t]):
            arrived(t, d, source)

            @pl.when(relayed(d))
            def _():
                for copy in relay(t, d, i, source):
                    copy.start()

    def lifts(t, d, pair, i, routes):
        return [
            (when, message(t, d, pair, block_at(shift, h), d_to, lift_send.at[t, d, i, k]))
            for k, (when, shift, d_to) in enumerate(routes)
        ]

    def lift(t, d, pair, i, routes):
        for when, copy in lifts(t, d, pair, i, routes):
            pl.when(when)(copy.start)

    def column(t, d):
        arrived(t, d, p)
        for copy in flat(t, d):
            copy.start()
        lift(t, d, p, 0, column_routes(d))

    def scores(c, d, line, version, causal, into, side):
        found = jnp.dot(
            k_buf[d, at(line * span, span, span), :], q_rot[version, c],
            preferred_element_type=jnp.float32,
        )
        if causal:
            key = lax.broadcasted_iota(jnp.int32, found.shape, 0)
            row = b * rows + lax.broadcasted_iota(jnp.int32, found.shape, 1)
            found = jnp.where(row >= key, found, MASKED)
        into[...] = found
        top[side] = jnp.max(found.reshape(span // 8, 8, rows), axis=0)

    def weigh(c, causal, source, into, side):
        new = jnp.max(top[side], axis=0, keepdims=True) * SCALE
        if causal:
            new = jnp.broadcast_to(new, (8, rows))
        else:
            old = peak[c]
            new = jnp.maximum(old, new)
            fade[side] = jnp.exp2(old - new)
        peak[c] = new
        new = new[:1]
        added = None
        for start in range(0, span, 64):
            weights = jnp.exp2(source[start : start + 64, :] * SCALE - new)
            some = jnp.sum(weights.reshape(8, 8, rows), axis=0)
            added = some if added is None else added + some
            into[start : start + 64, :] = weights.astype(jnp.bfloat16)
        total[c] = added if causal else total[c] * fade[side] + added

    def gather(c, d, line, causal, source, side):
        values = jnp.concatenate(
            [v_buf[d, line * side_b + i // 2, i % 2] for i in range(2 * side_b)], axis=1
        )
        product = jnp.dot(values, source[...], preferred_element_type=jnp.float32)
        acc[c] = product if causal else acc[c] * fade[side][:1] + product

    def attend(d, line, causal):
        version = jnp.minimum(d, 2)
        s_buf, w_buf = (s_even, s_odd), (w_even, w_odd)
        scores(0, d, line, version, causal, s_buf[0], 0)
        for c in range(CLUSTER):
            if c + 1 < CLUSTER:
                scores(c + 1, d, line, version, causal, s_buf[(c + 1) % 2], (c + 1) % 2)
            if c > 0:
                gather(c - 1, d, line, causal, w_buf[(c - 1) % 2], (c - 1) % 2)
            weigh(c, causal, s_buf[c % 2], w_buf[c % 2], c % 2)
        gather(CLUSTER - 1, d, line, causal, w_buf[(CLUSTER - 1) % 2], (CLUSTER - 1) % 2)

    query_swap.wait_recv()
    rotate_queries(lambda c: q_swap[:, c * HEAD_SIZE : (c + 1) * HEAD_SIZE], theirs)
    for t in range(2):
        pltpu.make_async_remote_copy(
            src_ref=(k_send, v_send)[t].at[h], dst_ref=part(t, 0, p, 1 - h),
            send_sem=swap_send.at[t], recv_sem=swap_recv.at[t],
            device_id=partner, device_id_type=mesh_type,
        ).wait_recv()

    for t in range(2):
        pass_on(t, 0)

        @pl.when(n > 0)
        def _():
            column(t, 1)

    for source in b_peers:
        arrived(1, 0, source)
    attend(0, a, True)

    def visit(j, carry):
        many = n >= 2
        most = n == last
        d = jnp.where(j < 2, 0, jnp.where((j == 2) | (j == 4), 1, 2))
        d = jnp.where((j == 3) & (n == 1), 1, d)
        d = jnp.where(((j == 5) & most) | (j == 7), last, d)
        across = (j == 1) | (j == 4) | (j > 5) | ((j == 3) & (n == 1)) | ((j == 5) & (n == 2))

        for t, d_in, stage, when in ((0, 2, 1, many), (0, last, 2, most), (1, last, 3, most)):
            @pl.when((j == stage) & when)
            def _():
                column(t, d_in)

        @pl.when(jnp.logical_not(across))
        def _():
            pass_on(0, d)
            for source in b_peers:
                arrived(1, d, source)
            pass_on(1, d)

        def cross(i, inner):
            line = (a + i) % side_a

            @pl.when(across)
            def _():
                for t in range(2):
                    @pl.when(t == 0)
                    def _():
                        arrived(t, d, pair_at(line, b))

                    for k in range(1, side_b):
                        pair = pair_at(line, (b + k) % side_b)
                        arrived(t, d, pair)

                        @pl.when(d == 0)
                        def _():
                            lift(t, 0, pair, (i - 1) * (side_b - 1) + k, diagonal_routes(0))

            @pl.when((j == 1) & many & (i == side_a - 1))
            def _():
                column(1, 2)

            @pl.when((d > 0) | (line < a))
            def _():
                attend(d, line, False)

            return inner

        return lax.fori_loop(
            jnp.where(across, 1, 0), jnp.where(across, side_a, 1), cross, carry
        )

    lax.fori_loop(1, 2 * (n + 1), visit, 0)

    def results(c):
        where = head_columns(h * CLUSTER + c)
        return (
            pltpu.make_async_copy(o_buf.at[c, mine, :], out.at[:, where], out_local.at[c]),
            pltpu.make_async_remote_copy(
                src_ref=o_buf.at[c, theirs, :], dst_ref=out.at[:, where],
                send_sem=out_send.at[c], recv_sem=out_recv.at[c],
                device_id=partner, device_id_type=mesh_type,
            ),
        )

    for c in range(CLUSTER + 1):
        if c < CLUSTER:
            share = 1.0 / jnp.sum(total[c], axis=0, keepdims=True)
            o_buf[c] = (acc[c] * share).astype(jnp.bfloat16).T
        if c > 0:
            for copy in results(c - 1):
                copy.start()

    query_swap.wait_send()
    for t in range(2):
        own, plain, lifted = firsts(t)
        own.wait_send()
        for copy in plain:
            copy.wait_send()
        for when, copy in lifted:
            pl.when(when)(copy.wait_send)

    for t in range(2):
        for d in range(BLOCKS):
            @pl.when(d <= n)
            def _():
                if d > 0:
                    for copy in flat(t, d):
                        copy.wait_send()
                    for when, copy in lifts(t, d, p, 0, column_routes(d)):
                        pl.when(when)(copy.wait_send)

                @pl.when(relayed(d))
                def _():
                    for i, source in enumerate((b_peers, a_peers)[t]):
                        for copy in relay(t, d, i, source):
                            copy.wait_send()

        for i, pair in enumerate(diagonal):
            for when, copy in lifts(t, 0, pair, 1 + i, diagonal_routes(0)):
                pl.when(when)(copy.wait_send)

    for c in range(CLUSTER):
        here, there = results(c)
        here.wait()
        there.wait_send()
        there.wait_recv()


def on_device(queries, keys, values):
    shard = queries.shape[0]
    pairs = lax.axis_size("seq") // 2
    sequences = lax.axis_size("stretch") // BLOCKS
    side_a = max(i for i in range(1, pairs + 1) if pairs % i == 0 and i * i <= pairs)
    side_b = pairs // side_a
    rows = 2 * shard
    length = pairs * rows
    span = side_b * rows
    shape = (shard, pairs, side_a, side_b, sequences, span)
    table = rotary_table(2 * length)
    far = np.broadcast_to(table[-1][:, None], (HEAD_SIZE, HEAD_SIZE))
    dma = pltpu.SemaphoreType.DMA
    peers = max(side_a - 1 + side_b - 1, 1)
    most = max(side_b - 1, side_a - 1, 1)
    lifted = 1 + (side_a - 1) * (side_b - 1)
    bf16, f32 = jnp.bfloat16, jnp.float32
    return pl.pallas_call(
        functools.partial(kernel, shape),
        out_shape=jax.ShapeDtypeStruct(queries.shape, bf16),
        in_specs=[pl.BlockSpec(memory_space=pl.ANY)] * 6,
        out_specs=pl.BlockSpec(memory_space=pl.ANY),
        scratch_shapes=[
            pltpu.VMEM((shard, 2 * WIDTH), bf16),
            pltpu.VMEM((shard, WIDTH), bf16),
            pltpu.VMEM((shard, 2 * HEAD_SIZE), bf16),
            pltpu.VMEM((shard, 2 * HEAD_SIZE), bf16),
            pltpu.VMEM((2, shard, HEAD_SIZE), bf16),
            pltpu.VMEM((2, HEAD_SIZE, shard), bf16),
            pltpu.VMEM((BLOCKS, length, HEAD_SIZE), bf16),
            pltpu.VMEM((BLOCKS, pairs, 2, HEAD_SIZE, shard), bf16),
            pltpu.VMEM((3, CLUSTER, HEAD_SIZE, rows), bf16),
            pltpu.VMEM((span, rows), f32),
            pltpu.VMEM((span, rows), f32),
            pltpu.VMEM((span, rows), bf16),
            pltpu.VMEM((span, rows), bf16),
            pltpu.VMEM((shard, HEAD_SIZE), f32),
            pltpu.VMEM((HEAD_SIZE, rows), f32),
            pltpu.VMEM((HEAD_SIZE, rows), f32),
            pltpu.VMEM((HEAD_SIZE, HEAD_SIZE), f32),
            pltpu.VMEM((CLUSTER, 8, rows), f32),
            pltpu.VMEM((CLUSTER, 8, rows), f32),
            pltpu.VMEM((2, 8, rows), f32),
            pltpu.VMEM((2, 8, rows), f32),
            pltpu.VMEM((CLUSTER, HEAD_SIZE, rows), f32),
            pltpu.VMEM((CLUSTER, rows, HEAD_SIZE), bf16),
            dma((7,)),
            dma((3,)),
            dma((3,)),
            dma((2, BLOCKS, pairs)),
            dma((2, 2, peers + 2)),
            dma((2, BLOCKS, peers)),
            dma((2, BLOCKS, most, most)),
            dma((2, BLOCKS, lifted, 2)),
            dma((CLUSTER,)),
            dma((CLUSTER,)),
            dma((CLUSTER,)),
        ],
        compiler_params=pltpu.CompilerParams(
            collective_id=0, has_side_effects=True, vmem_limit_bytes=60 * 1024 * 1024
        ),
    )(
        queries, keys, values,
        jnp.asarray(table[:length]), jnp.asarray(np.ascontiguousarray(table.T)), jnp.asarray(far),
    )


def solution(mesh):
    placed = P(("stretch", "seq"), None)
    return jax.shard_map(
        on_device, mesh=mesh, in_specs=(placed,) * 3, out_specs=placed, check_vma=False
    )
```

```python
import functools
import math

import jax
import jax.numpy as jnp
import numpy as np
from jax import lax
from jax.experimental import pallas as pl
from jax.experimental.pallas import tpu as pltpu
from jax.sharding import PartitionSpec as P

QUERY_HEADS = 14
KEY_VALUE_HEADS = 2
HEAD_SIZE = 128
BLOCKS = 4
CLUSTER = QUERY_HEADS // KEY_VALUE_HEADS
WIDTH = CLUSTER * HEAD_SIZE
HALF = HEAD_SIZE // 2
SCALE = math.log2(math.e) / math.sqrt(HEAD_SIZE)
MASKED = -1e30


def rotary_table(positions):
    inverse = 10000000.0 ** (-(np.arange(HALF, dtype=np.float64) * 2.0) / HEAD_SIZE)
    angles = np.arange(positions, dtype=np.float64)[:, None] * inverse[None, :]
    return np.concatenate([np.cos(angles), np.sin(angles)], axis=1).astype(np.float32)


def turned_rows(rows, table):
    swapped = pltpu.roll(table, HALF, 1)
    low = lax.broadcasted_iota(jnp.int32, table.shape, 1) < HALF
    cosine, sine = jnp.where(low, table, swapped), jnp.where(low, -swapped, table)
    x = rows.astype(jnp.float32)
    return (x * cosine + pltpu.roll(x, HALF, 1) * sine).astype(jnp.bfloat16)


def turned_columns(columns, table):
    x, y = columns[:HALF], columns[HALF:]
    cosine, sine = table[:HALF], table[HALF:]
    return jnp.concatenate([x * cosine - y * sine, y * cosine + x * sine], axis=0).astype(
        jnp.bfloat16
    )


def kernel(
    shape, q_in, k_in, v_in, rows_in, columns_in, far_in, out,
    q_own, q_swap, k_own, v_own, k_send, v_send, k_buf, v_buf, q_rot,
    s_even, s_odd, w_even, w_odd, row_table, near_tables, far_table,
    peak, total, fade, top, acc, o_buf,
    local_sem, swap_send, swap_recv, sent_sem, column_sem, near_sem, cross_sem, out_sem,
):
    shard, pairs, side_a, side_b, sequences, span = shape
    rows = 2 * shard
    length = pairs * rows
    s = lax.axis_index("seq")
    g = lax.axis_index("stretch")
    h = s % 2
    p = s // 2
    a = p // side_b
    b = p % side_b
    n = g // sequences
    last = BLOCKS - 1
    partner = {"seq": s + 1 - 2 * h}
    mesh_type = pl.DeviceIdType.MESH

    def pair_at(a_index, b_index):
        return a_index * side_b + b_index

    def device_at(pair, core):
        return {"seq": 2 * pair + core}

    def block_at(shift, core):
        return {"seq": 2 * p + core, "stretch": g + shift * sequences}

    a_peers = [pair_at((a + i) % side_a, b) for i in range(1, side_a)]
    b_peers = [pair_at(a, (b + j) % side_b) for j in range(1, side_b)]
    across_a, across_b = len(a_peers), len(b_peers)
    across = across_a * across_b

    def at(start, size, unit):
        return pl.ds(pl.multiple_of(start, unit), size)

    def half_columns(core):
        return at(core * shard, shard, shard)

    mine = half_columns(h)
    theirs = half_columns(1 - h)

    local = [
        (k_in, k_own, 0),
        (rows_in.at[at(p * rows + h * shard, shard, shard), :], row_table, 1),
        (v_in, v_own, 2),
        (q_in, q_own, 3),
        (columns_in.at[:, at(p * rows, rows, rows)], near_tables.at[0], 4),
        (columns_in.at[:, at(length + p * rows, rows, rows)], near_tables.at[1], 4),
        (far_in, far_table, 5),
    ]
    local = [pltpu.make_async_copy(src, dst, local_sem.at[i]) for src, dst, i in local]
    for copy in local:
        copy.start()

    barrier = pltpu.get_barrier_semaphore()

    def greet(device):
        pl.semaphore_signal(barrier, inc=1, device_id=device, device_id_type=mesh_type)

    for core in range(2):
        @pl.when(n < last)
        def _():
            greet(block_at(1, core))

        @pl.when(n > 0)
        def _():
            greet(block_at(-1, core))

        @pl.when((n == 0) | (n == last))
        def _():
            greet(partner)

        for peer in a_peers + b_peers:
            greet(device_at(peer, core))
    greet(partner)

    for copy in local[:3]:
        copy.wait()
    for head in range(KEY_VALUE_HEADS):
        columns = slice(head * HEAD_SIZE, (head + 1) * HEAD_SIZE)
        k_send[head] = turned_rows(k_own[:, columns], row_table[...])
        v_send[head] = v_own[:, columns].T

    def slot(t, d, pair):
        return (k_buf, v_buf)[t].at[pl.ds((d * pairs + pair) * 2, 2)]

    def place(d, pair, core):
        return (d * pairs + pair) * 2 + core

    k_buf[place(0, p, h)] = k_send[h]
    v_buf[place(0, p, h)] = v_send[h]
    local[3].wait()

    pl.semaphore_wait(barrier, 1 + 2 * (across_a + across_b) + 4)

    def send(src, dst, sent, received, device):
        return pltpu.make_async_remote_copy(
            src_ref=src, dst_ref=dst, send_sem=sent, recv_sem=received,
            device_id=device, device_id_type=mesh_type,
        )

    def halves(count):
        return k_buf.at[pl.ds(0, count)]

    def await_slots(count, received):
        some = halves(2 * count)
        send(some, some, swap_send, received, partner).wait_recv()

    def first(t, core, device, d_to, received):
        dst = (k_buf, v_buf)[t].at[place(d_to, p, h)]
        send((k_send, v_send)[t].at[core], dst, sent_sem.at[t, 0], received, device).start()

    def message(t, d, pair, device, d_to, group, received):
        src, dst = slot(t, d, pair), slot(t, d_to, pair)
        send(src, dst, sent_sem.at[t, group], received, device).start()

    def peers(t, d):
        to_a = cross_sem.at[d] if t == 0 else near_sem.at[1, d]
        return [(peer, near_sem.at[t, d]) for peer in b_peers] + [
            (peer, to_a) for peer in a_peers
        ]

    query_swap = send(
        q_own.at[:, at((1 - h) * WIDTH, WIDTH, HEAD_SIZE)], q_swap,
        swap_send, swap_recv.at[1], partner,
    )
    for t in range(2):
        for peer, received in peers(t, 0):
            for core in range(2):
                first(t, core, device_at(peer, core), 0, received)

        @pl.when(n < last)
        def _():
            for core in range(2):
                first(t, core, block_at(1, core), 1, column_sem.at[t, 1])

        first(t, 1 - h, partner, 0, swap_recv.at[0])
    query_swap.start()

    def column(t, d):
        await_slots(1, column_sem.at[t, d])
        for peer, received in peers(t, d):
            message(t, d, p, device_at(peer, h), d, 0, received)

        if not (isinstance(d, int) and d == last):
            @pl.when(n < last)
            def _():
                message(t, d, p, block_at(1, h), d + 1, 0, column_sem.at[t, d + 1])

    def relayed(d):
        return (d == 0) | (n < last) | (d == last)

    def pass_on(t, d):
        sources, targets = ((b_peers, a_peers), (a_peers, b_peers))[t]
        await_slots(across_b + t * across_a, near_sem.at[t, d])

        @pl.when(relayed(d))
        def _():
            for source in sources:
                for target in targets:
                    message(t, d, source, device_at(target, h), d, 1, cross_sem.at[d])

    def pass_up(d):
        for t in range(2):
            for i in range(1, side_a):
                for k in range(1, side_b):
                    pair = pair_at((a + i) % side_a, (b + k) % side_b)
                    message(t, d, pair, block_at(1, h), d + 1, 1, cross_sem.at[d + 1])

    def rotate_queries(source, half):
        near, later, far = near_tables[0, :, half], near_tables[1, :, half], far_table[:, :1]
        for c in range(CLUSTER):
            x = source(c).T.astype(jnp.float32)
            q_rot[0, c, :, half] = turned_columns(x, near)
            q_rot[1, c, :, half] = turned_columns(x, later)
            q_rot[2, c, :, half] = turned_columns(x, far)

    def scores(c, d, line, version, causal, into, side):
        keys = k_buf[pl.ds(place(d, line * side_b, 0), 2 * side_b)].reshape(span, HEAD_SIZE)
        found = jnp.dot(keys, q_rot[version, c], preferred_element_type=jnp.float32)
        if causal:
            key = lax.broadcasted_iota(jnp.int32, found.shape, 0)
            row = b * rows + lax.broadcasted_iota(jnp.int32, found.shape, 1)
            found = jnp.where(row >= key, found, MASKED)
        into[...] = found
        top[side] = jnp.max(found.reshape(span // 8, 8, rows), axis=0)

    def weigh(c, causal, source, into, side):
        new = jnp.max(top[side], axis=0, keepdims=True) * SCALE
        if causal:
            new = jnp.broadcast_to(new, (8, rows))
        else:
            old = peak[c]
            new = jnp.maximum(old, new)
            fade[side] = jnp.exp2(old - new)
        peak[c] = new
        new = new[:1]
        added = None
        for start in range(0, span, 64):
            weights = jnp.exp2(source[start : start + 64, :] * SCALE - new)
            some = jnp.sum(weights.reshape(8, 8, rows), axis=0)
            added = some if added is None else added + some
            into[start : start + 64, :] = weights.astype(jnp.bfloat16)
        total[c] = added if causal else total[c] * fade[side] + added

    def gather(c, d, line, causal, source, side):
        values = jnp.concatenate(
            [v_buf[place(d, line * side_b, i)] for i in range(2 * side_b)], axis=1
        )
        product = jnp.dot(values, source[...], preferred_element_type=jnp.float32)
        acc[c] = product if causal else acc[c] * fade[side][:1] + product

    def result(c):
        where = at((h * CLUSTER + c) * HEAD_SIZE, HEAD_SIZE, HEAD_SIZE)
        return send(
            o_buf.at[c, theirs, :], out.at[:, where], out_sem.at[0], out_sem.at[1], partner
        )

    def finish(c):
        share = 1.0 / jnp.sum(total[c], axis=0, keepdims=True)
        o_buf[c] = (acc[c] * share).astype(jnp.bfloat16).T
        out[:, at((h * CLUSTER + c) * HEAD_SIZE, HEAD_SIZE, HEAD_SIZE)] = o_buf[c, mine, :]

    def attend(d, line, causal, final):
        version = jnp.minimum(d, 2)
        s_buf, w_buf = (s_even, s_odd), (w_even, w_odd)
        scores(0, d, line, version, causal, s_buf[0], 0)
        for c in range(CLUSTER + 1):
            if c + 1 < CLUSTER:
                scores(c + 1, d, line, version, causal, s_buf[(c + 1) % 2], (c + 1) % 2)
            if c > 0:
                gather(c - 1, d, line, causal, w_buf[(c - 1) % 2], (c - 1) % 2)
                if final:
                    finish(c - 1)
                    if c > 1:
                        result(c - 2).start()
            if c < CLUSTER:
                weigh(c, causal, s_buf[c % 2], w_buf[c % 2], c % 2)
        if final:
            result(CLUSTER - 1).start()

    for copy in local[6:]:
        copy.wait()
    pltpu.make_async_copy(near_tables, near_tables, local_sem.at[4]).wait()
    rotate_queries(lambda c: q_own[:, at(h * WIDTH + c * HEAD_SIZE, HEAD_SIZE, HEAD_SIZE)], mine)
    query_swap.wait_recv()
    rotate_queries(lambda c: q_swap[:, c * HEAD_SIZE : (c + 1) * HEAD_SIZE], theirs)
    await_slots(1, swap_recv.at[0])

    for t in range(2):
        pass_on(t, 0)

        @pl.when(n > 0)
        def _():
            column(t, 1)

    attend(0, a, True, False)

    def cross(d):
        await_slots(across_a + 2 * across, cross_sem.at[d])

        @pl.when((n == last - 1) & (d < 2))
        def _():
            pass_up(d)

    def visit(j, carry):
        many = n >= 2
        most = n == last
        d = jnp.where(j < 2, 0, jnp.where((j == 2) | (j == 4), 1, 2))
        d = jnp.where((j == 3) & (n == 1), 1, d)
        d = jnp.where(((j == 5) & most) | (j == 7), last, d)
        other = (j == 1) | (j == 4) | (j > 5) | ((j == 3) & (n == 1)) | ((j == 5) & (n == 2))

        for t, d_in, stage, when in ((0, 2, 1, many), (0, last, 2, most), (1, last, 3, most)):
            @pl.when((j == stage) & when)
            def _():
                column(t, d_in)

        @pl.when(jnp.logical_not(other))
        def _():
            pass_on(0, d)
            pass_on(1, d)

        @pl.when(other)
        def _():
            cross(d)

        @pl.when((j == 1) & many)
        def _():
            column(1, 2)

        def inner(i, inside):
            line = (a + i) % side_a

            @pl.when((d > 0) | (line < a))
            def _():
                attend(d, line, False, False)

            return inside

        ends = jnp.where(other, side_a - jnp.where(j == 2 * n + 1, 1, 0), 1)
        return lax.fori_loop(jnp.where(other, 1, 0), ends, inner, carry)

    lax.fori_loop(1, 2 * (n + 1), visit, 0)
    line = (a + side_a - 1) % side_a
    reached = (n > 0) | (line < a)

    @pl.when(reached)
    def _():
        attend(n, line, False, True)

    @pl.when(jnp.logical_not(reached))
    def _():
        for c in range(CLUSTER + 1):
            if c < CLUSTER:
                finish(c)
            if c > 0:
                result(c - 1).start()

    query_swap.wait_send()
    for k in range(BLOCKS):
        lifted = 2 if k < last else 0
        direct = 2 * (across_a + across_b)
        counts = (
            direct + 1 + lifted + k * (direct + lifted),
            2 * across * (k + 1 if k < last else 2) + (4 * across if k == last - 1 else 0),
        )

        @pl.when(n == k)
        def _():
            for t in range(2):
                for group, count in enumerate(counts):
                    if count:
                        some = halves(count)
                        send(
                            some, some, sent_sem.at[t, group], swap_recv.at[0], partner
                        ).wait_send()

    whole = send(q_swap, q_swap, out_sem.at[0], out_sem.at[1], partner)
    whole.wait_send()
    whole.wait_recv()


def on_device(queries, keys, values):
    shard = queries.shape[0]
    pairs = lax.axis_size("seq") // 2
    sequences = lax.axis_size("stretch") // BLOCKS
    side_a = max(i for i in range(1, pairs + 1) if pairs % i == 0 and i * i <= pairs)
    side_b = pairs // side_a
    rows = 2 * shard
    length = pairs * rows
    span = side_b * rows
    shape = (shard, pairs, side_a, side_b, sequences, span)
    table = rotary_table(2 * length)
    far = np.broadcast_to(table[-1][:, None], (HEAD_SIZE, HEAD_SIZE))
    dma = pltpu.SemaphoreType.DMA
    bf16, f32 = jnp.bfloat16, jnp.float32
    return pl.pallas_call(
        functools.partial(kernel, shape),
        out_shape=pltpu.VMEM(queries.shape, bf16),
        in_specs=[pl.BlockSpec(memory_space=pl.ANY)] * 6,
        scratch_shapes=[
            pltpu.VMEM((shard, 2 * WIDTH), bf16),
            pltpu.VMEM((shard, WIDTH), bf16),
            pltpu.VMEM((shard, 2 * HEAD_SIZE), bf16),
            pltpu.VMEM((shard, 2 * HEAD_SIZE), bf16),
            pltpu.VMEM((2, shard, HEAD_SIZE), bf16),
            pltpu.VMEM((2, HEAD_SIZE, shard), bf16),
            pltpu.VMEM((BLOCKS * pairs * 2, shard, HEAD_SIZE), bf16),
            pltpu.VMEM((BLOCKS * pairs * 2, HEAD_SIZE, shard), bf16),
            pltpu.VMEM((3, CLUSTER, HEAD_SIZE, rows), bf16),
            pltpu.VMEM((span, rows), f32),
            pltpu.VMEM((span, rows), f32),
            pltpu.VMEM((span, rows), bf16),
            pltpu.VMEM((span, rows), bf16),
            pltpu.VMEM((shard, HEAD_SIZE), f32),
            pltpu.VMEM((2, HEAD_SIZE, rows), f32),
            pltpu.VMEM((HEAD_SIZE, HEAD_SIZE), f32),
            pltpu.VMEM((CLUSTER, 8, rows), f32),
            pltpu.VMEM((CLUSTER, 8, rows), f32),
            pltpu.VMEM((2, 8, rows), f32),
            pltpu.VMEM((2, 8, rows), f32),
            pltpu.VMEM((CLUSTER, HEAD_SIZE, rows), f32),
            pltpu.VMEM((CLUSTER, rows, HEAD_SIZE), bf16),
            dma((6,)),
            dma(()),
            dma((2,)),
            dma((2, 2)),
            dma((2, BLOCKS)),
            dma((2, BLOCKS)),
            dma((BLOCKS,)),
            dma((2,)),
        ],
        compiler_params=pltpu.CompilerParams(
            collective_id=0, has_side_effects=True, vmem_limit_bytes=60 * 1024 * 1024
        ),
    )(
        queries, keys, values,
        jnp.asarray(table[:length]), jnp.asarray(np.ascontiguousarray(table.T)), jnp.asarray(far),
    )


def solution(mesh):
    placed = P(("stretch", "seq"), None)
    return jax.shard_map(
        on_device, mesh=mesh, in_specs=(placed,) * 3, out_specs=placed, check_vma=False
    )
```

```python
import functools
import math

import jax
import jax.numpy as jnp
import numpy as np
from jax import lax
from jax.experimental import pallas as pl
from jax.experimental.pallas import tpu as pltpu
from jax.sharding import PartitionSpec as P

QUERY_HEADS = 14
KEY_VALUE_HEADS = 2
HEAD_SIZE = 128
BLOCKS = 4
CLUSTER = QUERY_HEADS // KEY_VALUE_HEADS
WIDTH = CLUSTER * HEAD_SIZE
HALF = HEAD_SIZE // 2
SCALE = math.log2(math.e) / math.sqrt(HEAD_SIZE)
MASKED = -1e30


def rotary_table(positions):
    inverse = 10000000.0 ** (-(np.arange(HALF, dtype=np.float64) * 2.0) / HEAD_SIZE)
    angles = np.arange(positions, dtype=np.float64)[:, None] * inverse[None, :]
    return np.concatenate([np.cos(angles), np.sin(angles)], axis=1).astype(np.float32)


def turned_rows(rows, table):
    swapped = pltpu.roll(table, HALF, 1)
    low = lax.broadcasted_iota(jnp.int32, table.shape, 1) < HALF
    cosine, sine = jnp.where(low, table, swapped), jnp.where(low, -swapped, table)
    x = rows.astype(jnp.float32)
    return (x * cosine + pltpu.roll(x, HALF, 1) * sine).astype(jnp.bfloat16)


def turned_columns(columns, table):
    x, y = columns[:HALF], columns[HALF:]
    cosine, sine = table[:HALF], table[HALF:]
    return jnp.concatenate([x * cosine - y * sine, y * cosine + x * sine], axis=0).astype(
        jnp.bfloat16
    )


def kernel(
    shape, q_in, k_in, v_in, rows_in, columns_in, far_in, out,
    q_own, q_swap, k_own, v_own, k_send, v_send, k_buf, v_buf, q_rot,
    s_even, s_odd, w_even, w_odd, row_table, near_tables, far_table,
    peak, total, fade, top, acc, o_buf,
    local_sem, swap_send, swap_recv, sent_sem, column_sem, near_sem, cross_sem, out_sem,
):
    shard, pairs, side_a, side_b, sequences, span = shape
    rows = 2 * shard
    length = pairs * rows
    s = lax.axis_index("seq")
    g = lax.axis_index("stretch")
    h = s % 2
    p = s // 2
    a = p // side_b
    b = p % side_b
    n = g // sequences
    last = BLOCKS - 1
    partner = {"seq": s + 1 - 2 * h}
    mesh_type = pl.DeviceIdType.MESH

    def pair_at(a_index, b_index):
        return a_index * side_b + b_index

    def device_at(pair, core):
        return {"seq": 2 * pair + core}

    def block_at(shift, core):
        return {"seq": 2 * p + core, "stretch": g + shift * sequences}

    a_peers = [pair_at((a + i) % side_a, b) for i in range(1, side_a)]
    b_peers = [pair_at(a, (b + j) % side_b) for j in range(1, side_b)]
    across_a, across_b = len(a_peers), len(b_peers)
    across = across_a * across_b

    def at(start, size, unit):
        return pl.ds(pl.multiple_of(start, unit), size)

    def half_columns(core):
        return at(core * shard, shard, shard)

    mine = half_columns(h)
    theirs = half_columns(1 - h)

    local = [
        (k_in, k_own, 0),
        (rows_in.at[at(p * rows + h * shard, shard, shard), :], row_table, 1),
        (v_in, v_own, 2),
        (q_in, q_own, 3),
        (columns_in.at[:, at(p * rows, rows, rows)], near_tables.at[0], 4),
        (columns_in.at[:, at(length + p * rows, rows, rows)], near_tables.at[1], 4),
        (far_in, far_table, 5),
    ]
    local = [pltpu.make_async_copy(src, dst, local_sem.at[i]) for src, dst, i in local]
    for copy in local:
        copy.start()

    barrier = pltpu.get_barrier_semaphore()

    def greet(device):
        pl.semaphore_signal(barrier, inc=1, device_id=device, device_id_type=mesh_type)

    for core in range(2):
        @pl.when(n < last)
        def _():
            greet(block_at(1, core))

        @pl.when(n > 0)
        def _():
            greet(block_at(-1, core))

        @pl.when((n == 0) | (n == last))
        def _():
            greet(partner)

        for peer in a_peers + b_peers:
            greet(device_at(peer, core))
    greet(partner)

    for copy in local[:3]:
        copy.wait()
    for head in range(KEY_VALUE_HEADS):
        columns = slice(head * HEAD_SIZE, (head + 1) * HEAD_SIZE)
        k_send[head] = turned_rows(k_own[:, columns], row_table[...])
        v_send[head] = v_own[:, columns].T

    def slot(t, d, pair):
        return (k_buf, v_buf)[t].at[pl.ds((d * pairs + pair) * 2, 2)]

    def place(d, pair, core):
        return (d * pairs + pair) * 2 + core

    k_buf[place(0, p, h)] = k_send[h]
    v_buf[place(0, p, h)] = v_send[h]
    local[3].wait()

    pl.semaphore_wait(barrier, 1 + 2 * (across_a + across_b) + 4)

    def send(src, dst, sent, received, device):
        return pltpu.make_async_remote_copy(
            src_ref=src, dst_ref=dst, send_sem=sent, recv_sem=received,
            device_id=device, device_id_type=mesh_type,
        )

    def halves(count):
        return k_buf.at[pl.ds(0, count)]

    def await_slots(count, received):
        some = halves(2 * count)
        send(some, some, swap_send, received, partner).wait_recv()

    def first(t, core, device, d_to, received):
        dst = (k_buf, v_buf)[t].at[place(d_to, p, h)]
        send((k_send, v_send)[t].at[core], dst, sent_sem.at[t, 0], received, device).start()

    def message(t, d, pair, device, d_to, group, received):
        src, dst = slot(t, d, pair), slot(t, d_to, pair)
        send(src, dst, sent_sem.at[t, group], received, device).start()

    def peers(t, d):
        to_a = cross_sem.at[d] if t == 0 else near_sem.at[1, d]
        return [(peer, near_sem.at[t, d]) for peer in b_peers] + [
            (peer, to_a) for peer in a_peers
        ]

    query_swap = send(
        q_own.at[:, at((1 - h) * WIDTH, WIDTH, HEAD_SIZE)], q_swap,
        swap_send, swap_recv.at[1], partner,
    )
    for t in range(2):
        for peer, received in peers(t, 0):
            for core in range(2):
                first(t, core, device_at(peer, core), 0, received)

        @pl.when(n < last)
        def _():
            for core in range(2):
                first(t, core, block_at(1, core), 1, column_sem.at[t, 1])

        first(t, 1 - h, partner, 0, swap_recv.at[0])
    query_swap.start()

    def column(t, d):
        await_slots(1, column_sem.at[t, d])
        for peer, received in peers(t, d):
            message(t, d, p, device_at(peer, h), d, 0, received)

        if not (isinstance(d, int) and d == last):
            @pl.when(n < last)
            def _():
                message(t, d, p, block_at(1, h), d + 1, 0, column_sem.at[t, d + 1])

    def relayed(d):
        return (d == 0) | (d == n - 1)

    def pass_on(t, d):
        sources, targets = ((b_peers, a_peers), (a_peers, b_peers))[t]
        await_slots(across_b + t * across_a, near_sem.at[t, d])

        @pl.when(relayed(d))
        def _():
            for source in sources:
                for target in targets:
                    message(t, d, source, device_at(target, h), d, 1, cross_sem.at[d])

    def pass_up(d):
        for t in range(2):
            for i in range(1, side_a):
                for k in range(1, side_b):
                    pair = pair_at((a + i) % side_a, (b + k) % side_b)
                    message(t, d, pair, block_at(1, h), d + 1, 1, cross_sem.at[d + 1])

    def rotate_queries(source, half):
        near, later, far = near_tables[0, :, half], near_tables[1, :, half], far_table[:, :1]
        for c in range(CLUSTER):
            x = source(c).T.astype(jnp.float32)
            q_rot[0, c, :, half] = turned_columns(x, near)
            q_rot[1, c, :, half] = turned_columns(x, later)
            q_rot[2, c, :, half] = turned_columns(x, far)

    def scores(c, d, line, version, causal, into, side):
        keys = k_buf[pl.ds(place(d, line * side_b, 0), 2 * side_b)].reshape(span, HEAD_SIZE)
        found = jnp.dot(keys, q_rot[version, c], preferred_element_type=jnp.float32)
        if causal:
            key = lax.broadcasted_iota(jnp.int32, found.shape, 0)
            row = b * rows + lax.broadcasted_iota(jnp.int32, found.shape, 1)
            found = jnp.where(row >= key, found, MASKED)
        into[...] = found
        top[side] = jnp.max(found.reshape(span // 8, 8, rows), axis=0)

    def weigh(c, causal, source, into, side):
        new = jnp.max(top[side], axis=0, keepdims=True) * SCALE
        if causal:
            new = jnp.broadcast_to(new, (8, rows))
        else:
            old = peak[c]
            new = jnp.maximum(old, new)
            fade[side] = jnp.exp2(old - new)
        peak[c] = new
        new = new[:1]
        added = None
        for start in range(0, span, 64):
            weights = jnp.exp2(source[start : start + 64, :] * SCALE - new)
            some = jnp.sum(weights.reshape(8, 8, rows), axis=0)
            added = some if added is None else added + some
            into[start : start + 64, :] = weights.astype(jnp.bfloat16)
        total[c] = added if causal else total[c] * fade[side] + added

    def gather(c, d, line, causal, source, side):
        values = jnp.concatenate(
            [v_buf[place(d, line * side_b, i)] for i in range(2 * side_b)], axis=1
        )
        product = jnp.dot(values, source[...], preferred_element_type=jnp.float32)
        acc[c] = product if causal else acc[c] * fade[side][:1] + product

    def result(c):
        where = at((h * CLUSTER + c) * HEAD_SIZE, HEAD_SIZE, HEAD_SIZE)
        return send(
            o_buf.at[c, theirs, :], out.at[:, where], out_sem.at[0], out_sem.at[1], partner
        )

    def finish(c):
        share = 1.0 / jnp.sum(total[c], axis=0, keepdims=True)
        o_buf[c] = (acc[c] * share).astype(jnp.bfloat16).T
        out[:, at((h * CLUSTER + c) * HEAD_SIZE, HEAD_SIZE, HEAD_SIZE)] = o_buf[c, mine, :]

    def attend(d, line, causal, final):
        version = jnp.minimum(d, 2)
        s_buf, w_buf = (s_even, s_odd), (w_even, w_odd)
        scores(0, d, line, version, causal, s_buf[0], 0)
        for c in range(CLUSTER + 1):
            if c + 1 < CLUSTER:
                scores(c + 1, d, line, version, causal, s_buf[(c + 1) % 2], (c + 1) % 2)
            if c > 0:
                gather(c - 1, d, line, causal, w_buf[(c - 1) % 2], (c - 1) % 2)
                if final:
                    finish(c - 1)
                    if c > 1:
                        result(c - 2).start()
            if c < CLUSTER:
                weigh(c, causal, s_buf[c % 2], w_buf[c % 2], c % 2)
        if final:
            result(CLUSTER - 1).start()

    for copy in local[6:]:
        copy.wait()
    pltpu.make_async_copy(near_tables, near_tables, local_sem.at[4]).wait()
    rotate_queries(lambda c: q_own[:, at(h * WIDTH + c * HEAD_SIZE, HEAD_SIZE, HEAD_SIZE)], mine)
    query_swap.wait_recv()
    rotate_queries(lambda c: q_swap[:, c * HEAD_SIZE : (c + 1) * HEAD_SIZE], theirs)
    await_slots(1, swap_recv.at[0])

    for t in range(2):
        pass_on(t, 0)

        @pl.when(n > 0)
        def _():
            column(t, 1)

    attend(0, a, True, False)

    def cross(d):
        await_slots(across_a + 2 * across, cross_sem.at[d])

        @pl.when(((n < last) & (d == n)) | ((n == last - 1) & (d == 0)))
        def _():
            pass_up(d)

    def visit(j, carry):
        many = n >= 2
        most = n == last
        d = jnp.where(j < 2, 0, jnp.where((j == 2) | (j == 4), 1, 2))
        d = jnp.where((j == 3) & (n == 1), 1, d)
        d = jnp.where(((j == 5) & most) | (j == 7), last, d)
        other = (j == 1) | (j == 4) | (j > 5) | ((j == 3) & (n == 1)) | ((j == 5) & (n == 2))

        for t, d_in, stage, when in ((0, 2, 1, many), (0, last, 2, most), (1, last, 3, most)):
            @pl.when((j == stage) & when)
            def _():
                column(t, d_in)

        @pl.when(jnp.logical_not(other))
        def _():
            pass_on(0, d)
            pass_on(1, d)

        @pl.when((j == 1) & many)
        def _():
            column(1, 2)

        @pl.when(other)
        def _():
            cross(d)

        def inner(i, inside):
            line = (a + i) % side_a

            @pl.when((d > 0) | (line < a))
            def _():
                attend(d, line, False, False)

            return inside

        ends = jnp.where(other, side_a - jnp.where(j == 2 * n + 1, 1, 0), 1)
        return lax.fori_loop(jnp.where(other, 1, 0), ends, inner, carry)

    lax.fori_loop(1, 2 * (n + 1), visit, 0)
    line = (a + side_a - 1) % side_a
    reached = (n > 0) | (line < a)

    @pl.when(reached)
    def _():
        attend(n, line, False, True)

    @pl.when(jnp.logical_not(reached))
    def _():
        for c in range(CLUSTER + 1):
            if c < CLUSTER:
                finish(c)
            if c > 0:
                result(c - 1).start()

    query_swap.wait_send()
    for k in range(BLOCKS):
        lifted = 2 if k < last else 0
        direct = 2 * (across_a + across_b)
        counts = (
            direct + 1 + lifted + k * (direct + lifted),
            2 * across * ((2 if k > 1 else 1) + (k < last) + (k == last - 1)),
        )

        @pl.when(n == k)
        def _():
            for t in range(2):
                for group, count in enumerate(counts):
                    if count:
                        some = halves(count)
                        send(
                            some, some, sent_sem.at[t, group], swap_recv.at[0], partner
                        ).wait_send()

    whole = send(q_swap, q_swap, out_sem.at[0], out_sem.at[1], partner)
    whole.wait_send()
    whole.wait_recv()


def on_device(queries, keys, values):
    shard = queries.shape[0]
    pairs = lax.axis_size("seq") // 2
    sequences = lax.axis_size("stretch") // BLOCKS
    side_a = max(i for i in range(1, pairs + 1) if pairs % i == 0 and i * i <= pairs)
    side_b = pairs // side_a
    rows = 2 * shard
    length = pairs * rows
    span = side_b * rows
    shape = (shard, pairs, side_a, side_b, sequences, span)
    table = rotary_table(2 * length)
    far = np.broadcast_to(table[-1][:, None], (HEAD_SIZE, HEAD_SIZE))
    dma = pltpu.SemaphoreType.DMA
    bf16, f32 = jnp.bfloat16, jnp.float32
    return pl.pallas_call(
        functools.partial(kernel, shape),
        out_shape=pltpu.VMEM(queries.shape, bf16),
        in_specs=[pl.BlockSpec(memory_space=pl.ANY)] * 6,
        scratch_shapes=[
            pltpu.VMEM((shard, 2 * WIDTH), bf16),
            pltpu.VMEM((shard, WIDTH), bf16),
            pltpu.VMEM((shard, 2 * HEAD_SIZE), bf16),
            pltpu.VMEM((shard, 2 * HEAD_SIZE), bf16),
            pltpu.VMEM((2, shard, HEAD_SIZE), bf16),
            pltpu.VMEM((2, HEAD_SIZE, shard), bf16),
            pltpu.VMEM((BLOCKS * pairs * 2, shard, HEAD_SIZE), bf16),
            pltpu.VMEM((BLOCKS * pairs * 2, HEAD_SIZE, shard), bf16),
            pltpu.VMEM((3, CLUSTER, HEAD_SIZE, rows), bf16),
            pltpu.VMEM((span, rows), f32),
            pltpu.VMEM((span, rows), f32),
            pltpu.VMEM((span, rows), bf16),
            pltpu.VMEM((span, rows), bf16),
            pltpu.VMEM((shard, HEAD_SIZE), f32),
            pltpu.VMEM((2, HEAD_SIZE, rows), f32),
            pltpu.VMEM((HEAD_SIZE, HEAD_SIZE), f32),
            pltpu.VMEM((CLUSTER, 8, rows), f32),
            pltpu.VMEM((CLUSTER, 8, rows), f32),
            pltpu.VMEM((2, 8, rows), f32),
            pltpu.VMEM((2, 8, rows), f32),
            pltpu.VMEM((CLUSTER, HEAD_SIZE, rows), f32),
            pltpu.VMEM((CLUSTER, rows, HEAD_SIZE), bf16),
            dma((6,)),
            dma(()),
            dma((2,)),
            dma((2, 2)),
            dma((2, BLOCKS)),
            dma((2, BLOCKS)),
            dma((BLOCKS,)),
            dma((2,)),
        ],
        compiler_params=pltpu.CompilerParams(
            collective_id=0, has_side_effects=True, vmem_limit_bytes=60 * 1024 * 1024
        ),
    )(
        queries, keys, values,
        jnp.asarray(table[:length]), jnp.asarray(np.ascontiguousarray(table.T)), jnp.asarray(far),
    )


def solution(mesh):
    placed = P(("stretch", "seq"), None)
    return jax.shard_map(
        on_device, mesh=mesh, in_specs=(placed,) * 3, out_specs=placed, check_vma=False
    )
```

```python
import functools
import math

import jax
import jax.numpy as jnp
import numpy as np
from jax import lax
from jax.experimental import pallas as pl
from jax.experimental.pallas import tpu as pltpu
from jax.sharding import PartitionSpec as P

QUERY_HEADS = 14
KEY_VALUE_HEADS = 2
HEAD_SIZE = 128
BLOCKS = 4
CLUSTER = QUERY_HEADS // KEY_VALUE_HEADS
WIDTH = CLUSTER * HEAD_SIZE
HALF = HEAD_SIZE // 2
SCALE = math.log2(math.e) / math.sqrt(HEAD_SIZE)
MASKED = -1e30


def rotary_table(positions):
    inverse = 10000000.0 ** (-(np.arange(HALF, dtype=np.float64) * 2.0) / HEAD_SIZE)
    angles = np.arange(positions, dtype=np.float64)[:, None] * inverse[None, :]
    return np.concatenate([np.cos(angles), np.sin(angles)], axis=1).astype(np.float32)


def turned_rows(rows, table):
    swapped = pltpu.roll(table, HALF, 1)
    low = lax.broadcasted_iota(jnp.int32, table.shape, 1) < HALF
    cosine, sine = jnp.where(low, table, swapped), jnp.where(low, -swapped, table)
    x = rows.astype(jnp.float32)
    return (x * cosine + pltpu.roll(x, HALF, 1) * sine).astype(jnp.bfloat16)


def turned_columns(columns, table):
    x, y = columns[:HALF], columns[HALF:]
    cosine, sine = table[:HALF], table[HALF:]
    return jnp.concatenate([x * cosine - y * sine, y * cosine + x * sine], axis=0).astype(
        jnp.bfloat16
    )


def kernel(
    shape, q_in, k_in, v_in, rows_in, columns_in, far_in, out,
    q_own, q_swap, k_own, v_own, k_send, v_send, k_buf, v_buf, q_rot,
    s_even, s_odd, w_even, w_odd, row_table, near_tables, far_table,
    peak, total, fade, top, acc, o_buf,
    local_sem, swap_send, swap_recv, sent_sem, column_sem, near_sem, cross_sem, out_sem,
):
    shard, pairs, side_a, side_b, sequences, span = shape
    rows = 2 * shard
    length = pairs * rows
    s = lax.axis_index("seq")
    g = lax.axis_index("stretch")
    h = s % 2
    p = s // 2
    a = p // side_b
    b = p % side_b
    n = g // sequences
    last = BLOCKS - 1
    partner = {"seq": s + 1 - 2 * h}
    mesh_type = pl.DeviceIdType.MESH

    def pair_at(a_index, b_index):
        return a_index * side_b + b_index

    def device_at(pair, core):
        return {"seq": 2 * pair + core}

    def block_at(shift, core):
        return {"seq": 2 * p + core, "stretch": g + shift * sequences}

    a_peers = [pair_at((a + i) % side_a, b) for i in range(1, side_a)]
    b_peers = [pair_at(a, (b + j) % side_b) for j in range(1, side_b)]
    diagonal = [
        pair_at((a + i) % side_a, (b + j) % side_b)
        for i in range(1, side_a)
        for j in range(1, side_b)
    ]
    across_a, across_b = len(a_peers), len(b_peers)
    across = across_a * across_b

    def at(start, size, unit):
        return pl.ds(pl.multiple_of(start, unit), size)

    def half_columns(core):
        return at(core * shard, shard, shard)

    mine = half_columns(h)
    theirs = half_columns(1 - h)

    local = [
        (k_in, k_own, 0),
        (rows_in.at[at(p * rows + h * shard, shard, shard), :], row_table, 1),
        (v_in, v_own, 2),
        (q_in, q_own, 3),
        (columns_in.at[:, at(p * rows, rows, rows)], near_tables.at[0], 4),
        (columns_in.at[:, at(length + p * rows, rows, rows)], near_tables.at[1], 4),
        (far_in, far_table, 5),
    ]
    local = [pltpu.make_async_copy(src, dst, local_sem.at[i]) for src, dst, i in local]
    for copy in local:
        copy.start()

    barrier = pltpu.get_barrier_semaphore()

    def greet(device):
        pl.semaphore_signal(barrier, inc=1, device_id=device, device_id_type=mesh_type)

    for core in range(2):
        @pl.when(n < last)
        def _():
            greet(block_at(1, core))

        @pl.when(n > 0)
        def _():
            greet(block_at(-1, core))

        @pl.when((n == 0) | (n == last))
        def _():
            greet(partner)

        for peer in a_peers + b_peers:
            greet(device_at(peer, core))
    greet(partner)

    for copy in local[:3]:
        copy.wait()
    for head in range(KEY_VALUE_HEADS):
        columns = slice(head * HEAD_SIZE, (head + 1) * HEAD_SIZE)
        k_send[head] = turned_rows(k_own[:, columns], row_table[...])
        v_send[head] = v_own[:, columns].T

    def slot(t, d, pair):
        return (k_buf, v_buf)[t].at[pl.ds((d * pairs + pair) * 2, 2)]

    def place(d, pair, core):
        return (d * pairs + pair) * 2 + core

    k_buf[place(0, p, h)] = k_send[h]
    v_buf[place(0, p, h)] = v_send[h]
    pl.semaphore_wait(barrier, 1 + 2 * (across_a + across_b) + 4)

    def send(src, dst, sent, received, device):
        return pltpu.make_async_remote_copy(
            src_ref=src, dst_ref=dst, send_sem=sent, recv_sem=received,
            device_id=device, device_id_type=mesh_type,
        )

    def halves(count):
        return k_buf.at[pl.ds(0, count)]

    def await_slots(count, received):
        some = halves(2 * count)
        send(some, some, swap_send, received, partner).wait_recv()

    def first(t, core, device, d_to, received):
        dst = (k_buf, v_buf)[t].at[place(d_to, p, h)]
        send((k_send, v_send)[t].at[core], dst, sent_sem.at[t, 0], received, device).start()

    def message(t, d, pair, device, d_to, group, received):
        src, dst = slot(t, d, pair), slot(t, d_to, pair)
        send(src, dst, sent_sem.at[t, group], received, device).start()

    def peers(t, d):
        return [(peer, near_sem.at[t, d]) for peer in b_peers + a_peers]

    query_swap = send(
        q_own.at[:, at((1 - h) * WIDTH, WIDTH, HEAD_SIZE)], q_swap,
        swap_send, swap_recv.at[1], partner,
    )
    for t in range(2):
        for peer, received in peers(t, 0):
            for core in range(2):
                first(t, core, device_at(peer, core), 0, received)

        @pl.when(n < last)
        def _():
            for core in range(2):
                first(t, core, block_at(1, core), 1, column_sem.at[t, 1])

        first(t, 1 - h, partner, 0, swap_recv.at[0])
    local[3].wait()
    query_swap.start()

    def column(t, d):
        await_slots(1, column_sem.at[t, d])
        for peer, received in peers(t, d):
            message(t, d, p, device_at(peer, h), d, 0, received)

        if not (isinstance(d, int) and d == last):
            @pl.when(n < last)
            def _():
                message(t, d, p, block_at(1, h), d + 1, 0, column_sem.at[t, d + 1])

    def relayed(d):
        return (d == 0) | (d == n - 1)

    def pass_on(t, d):
        sources, targets = ((b_peers, a_peers), (a_peers, b_peers))[t]
        await_slots(across_a + across_b, near_sem.at[t, d])

        @pl.when(relayed(d))
        def _():
            for source in sources:
                for target in targets:
                    message(t, d, source, device_at(target, h), d, 1, cross_sem.at[t, d])

    def cross(d):
        for t in range(2):
            await_slots(across, cross_sem.at[t, d])

            @pl.when(((n < last) & (n == d)) | ((n == last - 1) & (d == 0)))
            def _():
                for pair in diagonal:
                    message(t, d, pair, block_at(1, h), d + 1, 1, cross_sem.at[t, d + 1])

    def rotate_queries(source, half):
        near, later, far = near_tables[0, :, half], near_tables[1, :, half], far_table[:, :1]
        for c in range(CLUSTER):
            x = source(c).T.astype(jnp.float32)
            for version, table in enumerate((near, later, far)):
                scaled = turned_columns(x, table).astype(jnp.float32) * SCALE
                high = scaled.astype(jnp.bfloat16)
                q_rot[version, c, :HEAD_SIZE, half] = high
                rest = scaled - high.astype(jnp.float32)
                q_rot[version, c, HEAD_SIZE:, half] = rest.astype(jnp.bfloat16)

    def scores(c, starts, version, causal, into, side):
        keys = jnp.concatenate(
            [k_buf[pl.ds(start, 2)].reshape(rows, HEAD_SIZE) for start in starts], axis=0
        )
        keys = jnp.concatenate([keys, keys], axis=1)
        found = jnp.dot(keys, q_rot[version, c], preferred_element_type=jnp.float32)
        if causal:
            key = lax.broadcasted_iota(jnp.int32, found.shape, 0)
            row = b * rows + lax.broadcasted_iota(jnp.int32, found.shape, 1)
            found = jnp.where(row >= key, found, MASKED)
        into[...] = found
        top[side] = jnp.max(found.reshape(span // 8, 8, rows), axis=0)

    def weigh(c, causal, source, into, side):
        new = jnp.max(top[side], axis=0, keepdims=True)
        if causal:
            new = jnp.broadcast_to(new, (8, rows))
        else:
            old = peak[c]
            new = jnp.maximum(old, new)
            fade[side] = jnp.exp2(old - new)
        peak[c] = new
        new = new[:1]
        added = None
        for start in range(0, span, 64):
            weights = jnp.exp2(source[start : start + 64, :] - new)
            some = jnp.sum(weights.reshape(8, 8, rows), axis=0)
            added = some if added is None else added + some
            into[start : start + 64, :] = weights.astype(jnp.bfloat16)
        total[c] = added if causal else total[c] * fade[side] + added

    def gather(c, starts, causal, source, side):
        values = jnp.concatenate(
            [v_buf[start + i] for start in starts for i in range(2)], axis=1
        )
        product = jnp.dot(values, source[...], preferred_element_type=jnp.float32)
        acc[c] = product if causal else acc[c] * fade[side][:1] + product

    def result(c):
        where = at((h * CLUSTER + c) * HEAD_SIZE, HEAD_SIZE, HEAD_SIZE)
        return send(
            o_buf.at[c, theirs, :], out.at[:, where], out_sem.at[0], out_sem.at[1], partner
        )

    def finish(c):
        share = 1.0 / jnp.sum(total[c], axis=0, keepdims=True)
        o_buf[c] = (acc[c] * share).astype(jnp.bfloat16).T
        out[:, at((h * CLUSTER + c) * HEAD_SIZE, HEAD_SIZE, HEAD_SIZE)] = o_buf[c, mine, :]

    def in_line(d, line):
        return [place(d, line * side_b + i, 0) for i in range(side_b)]

    def attend(starts, version, causal, final):
        s_buf, w_buf = (s_even, s_odd), (w_even, w_odd)
        scores(0, starts, version, causal, s_buf[0], 0)
        for c in range(CLUSTER + 1):
            if c + 1 < CLUSTER:
                scores(c + 1, starts, version, causal, s_buf[(c + 1) % 2], (c + 1) % 2)
            if c > 0:
                gather(c - 1, starts, causal, w_buf[(c - 1) % 2], (c - 1) % 2)
                if final:
                    finish(c - 1)
                    if c > 1:
                        result(c - 2).start()
            if c < CLUSTER:
                weigh(c, causal, s_buf[c % 2], w_buf[c % 2], c % 2)
        if final:
            result(CLUSTER - 1).start()

    for copy in local[6:]:
        copy.wait()
    pltpu.make_async_copy(near_tables, near_tables, local_sem.at[4]).wait()
    rotate_queries(lambda c: q_own[:, at(h * WIDTH + c * HEAD_SIZE, HEAD_SIZE, HEAD_SIZE)], mine)
    query_swap.wait_recv()
    rotate_queries(lambda c: q_swap[:, c * HEAD_SIZE : (c + 1) * HEAD_SIZE], theirs)
    await_slots(1, swap_recv.at[0])

    for t in range(2):
        pass_on(t, 0)

        @pl.when(n > 0)
        def _():
            column(t, 1)

    attend(in_line(0, a), 0, True, False)

    many = n >= 2
    most = n == last
    square = side_a == 2 and side_b == 2

    def choose(j, *pairs):
        found = pairs[-1]
        for when, value in reversed(pairs[:-1]):
            found = jnp.where((j == when), value, found)
        return found

    def visit(j, carry):
        d = jnp.where(j < 2, 0, jnp.where((j == 2) | (j == 4), 1, 2))
        d = jnp.where((j == 3) & (n == 1), 1, d)
        d = jnp.where(((j == 5) & most) | (j == 7), last, d)
        other = (j == 1) | (j == 4) | (j > 5) | ((j == 3) & (n == 1)) | ((j == 5) & (n == 2))
        near = jnp.logical_not(other)
        if square:
            d = jnp.where(most, choose(j, (1, 0), (4, 2), (6, 3), (3, 2), (7, 2), 1), d)
            other = jnp.where(most, ((j == 1) | (j == 5)).astype(jnp.int32), other.astype(jnp.int32)) == 1
            near = (most & (j % 2 == 0)) | (jnp.logical_not(most) & near)

        for t, d_in, stage, when in (
            (0, 2, 1, many), (1, 2, 1, many), (0, last, 2, most), (1, last, 3, most)
        ):
            @pl.when((j == stage) & when)
            def _():
                column(t, d_in)

        @pl.when(near)
        def _():
            pass_on(0, d)
            pass_on(1, d)

        late = ((1, 5), (2, 7), (last, 7)) if square else ((1, 4), (2, 6), (last, 7))
        for d_in, stage, when in [(0, 1, n >= 0), (1, 2, n == 1), (2, 3, n == 2), (1, 4, n == 2)] + [
            (d_in, stage, most) for d_in, stage in late
        ]:
            @pl.when((j == stage) & when)
            def _():
                cross(d_in)

        def inner(i, inside):
            line = (a + i) % side_a
            starts = in_line(d, line)
            if square:
                pick = [
                    [place(2, p, 0), place(last, p, 0)],
                    [place(2, b_peers[0], 0), place(2, a_peers[0], 0)],
                    [place(last, b_peers[0], 0), place(last, a_peers[0], 0)],
                ]
                starts = [
                    jnp.where(most, choose(j, *zip((3, 4, 6), options), start), start)
                    for start, *options in zip(starts, *pick)
                ]

            @pl.when((d > 0) | (line < a))
            def _():
                attend(starts, jnp.minimum(d, 2), False, False)

            return inside

        ends = jnp.where(other, side_a, 1) - jnp.where(j == 2 * n + 1, 1, 0)
        begins = jnp.where(other, 1, 0)
        return lax.fori_loop(begins, ends, inner, carry)

    lax.fori_loop(1, 2 * (n + 1), visit, 0)
    line = (a + side_a - 1) % side_a
    reached = (n > 0) | (line < a)
    starts = in_line(n, line)
    if square:
        options = [place(2, diagonal[0], 0), place(last, diagonal[0], 0)]
        starts = [jnp.where(most, option, start) for option, start in zip(options, starts)]

    @pl.when(reached)
    def _():
        attend(starts, jnp.minimum(n, 2), False, True)

    @pl.when(jnp.logical_not(reached))
    def _():
        for c in range(CLUSTER + 1):
            if c < CLUSTER:
                finish(c)
            if c > 0:
                result(c - 1).start()

    query_swap.wait_send()
    for k in range(BLOCKS):
        lifted = 2 if k < last else 0
        direct = 2 * (across_a + across_b)
        counts = (
            direct + 1 + lifted + k * (direct + lifted),
            2 * across * ((2 if k > 1 else 1) + (k < last) + (k == last - 1)),
        )

        @pl.when(n == k)
        def _():
            for t in range(2):
                for group, count in enumerate(counts):
                    if count:
                        some = halves(count)
                        send(
                            some, some, sent_sem.at[t, group], swap_recv.at[0], partner
                        ).wait_send()

    whole = send(q_swap, q_swap, out_sem.at[0], out_sem.at[1], partner)
    whole.wait_send()
    whole.wait_recv()


def on_device(queries, keys, values):
    shard = queries.shape[0]
    pairs = lax.axis_size("seq") // 2
    sequences = lax.axis_size("stretch") // BLOCKS
    side_a = max(i for i in range(1, pairs + 1) if pairs % i == 0 and i * i <= pairs)
    side_b = pairs // side_a
    rows = 2 * shard
    length = pairs * rows
    span = side_b * rows
    shape = (shard, pairs, side_a, side_b, sequences, span)
    table = rotary_table(2 * length)
    far = np.broadcast_to(table[-1][:, None], (HEAD_SIZE, HEAD_SIZE))
    dma = pltpu.SemaphoreType.DMA
    bf16, f32 = jnp.bfloat16, jnp.float32
    return pl.pallas_call(
        functools.partial(kernel, shape),
        out_shape=pltpu.VMEM(queries.shape, bf16),
        in_specs=[pl.BlockSpec(memory_space=pl.ANY)] * 6,
        scratch_shapes=[
            pltpu.VMEM((shard, 2 * WIDTH), bf16),
            pltpu.VMEM((shard, WIDTH), bf16),
            pltpu.VMEM((shard, 2 * HEAD_SIZE), bf16),
            pltpu.VMEM((shard, 2 * HEAD_SIZE), bf16),
            pltpu.VMEM((2, shard, HEAD_SIZE), bf16),
            pltpu.VMEM((2, HEAD_SIZE, shard), bf16),
            pltpu.VMEM((BLOCKS * pairs * 2, shard, HEAD_SIZE), bf16),
            pltpu.VMEM((BLOCKS * pairs * 2, HEAD_SIZE, shard), bf16),
            pltpu.VMEM((3, CLUSTER, 2 * HEAD_SIZE, rows), bf16),
            pltpu.VMEM((span, rows), f32),
            pltpu.VMEM((span, rows), f32),
            pltpu.VMEM((span, rows), bf16),
            pltpu.VMEM((span, rows), bf16),
            pltpu.VMEM((shard, HEAD_SIZE), f32),
            pltpu.VMEM((2, HEAD_SIZE, rows), f32),
            pltpu.VMEM((HEAD_SIZE, HEAD_SIZE), f32),
            pltpu.VMEM((CLUSTER, 8, rows), f32),
            pltpu.VMEM((CLUSTER, 8, rows), f32),
            pltpu.VMEM((2, 8, rows), f32),
            pltpu.VMEM((2, 8, rows), f32),
            pltpu.VMEM((CLUSTER, HEAD_SIZE, rows), f32),
            pltpu.VMEM((CLUSTER, rows, HEAD_SIZE), bf16),
            dma((6,)),
            dma(()),
            dma((2,)),
            dma((2, 2)),
            dma((2, BLOCKS)),
            dma((2, BLOCKS)),
            dma((2, BLOCKS)),
            dma((2,)),
        ],
        compiler_params=pltpu.CompilerParams(
            collective_id=0, has_side_effects=True, vmem_limit_bytes=60 * 1024 * 1024
        ),
    )(
        queries, keys, values,
        jnp.asarray(table[:length]), jnp.asarray(np.ascontiguousarray(table.T)), jnp.asarray(far),
    )


def solution(mesh):
    placed = P(("stretch", "seq"), None)
    return jax.shard_map(
        on_device, mesh=mesh, in_specs=(placed,) * 3, out_specs=placed, check_vma=False
    )
```

```python
import functools
import math

import jax
import jax.numpy as jnp
import numpy as np
from jax import lax
from jax.experimental import pallas as pl
from jax.experimental.pallas import tpu as pltpu
from jax.sharding import PartitionSpec as P

QUERY_HEADS = 14
KEY_VALUE_HEADS = 2
HEAD_SIZE = 128
BLOCKS = 4
CLUSTER = QUERY_HEADS // KEY_VALUE_HEADS
WIDTH = CLUSTER * HEAD_SIZE
HALF = HEAD_SIZE // 2
SCALE = math.log2(math.e) / math.sqrt(HEAD_SIZE)
MASKED = -1e30


def rotary_table(positions):
    inverse = 10000000.0 ** (-(np.arange(HALF, dtype=np.float64) * 2.0) / HEAD_SIZE)
    angles = np.arange(positions, dtype=np.float64)[:, None] * inverse[None, :]
    return np.concatenate([np.cos(angles), np.sin(angles)], axis=1).astype(np.float32)


def turned_rows(rows, table):
    swapped = pltpu.roll(table, HALF, 1)
    low = lax.broadcasted_iota(jnp.int32, table.shape, 1) < HALF
    cosine, sine = jnp.where(low, table, swapped), jnp.where(low, -swapped, table)
    x = rows.astype(jnp.float32)
    return (x * cosine + pltpu.roll(x, HALF, 1) * sine).astype(jnp.bfloat16)


def turned_columns(columns, table):
    x, y = columns[:HALF], columns[HALF:]
    cosine, sine = table[:HALF], table[HALF:]
    return jnp.concatenate([x * cosine - y * sine, y * cosine + x * sine], axis=0).astype(
        jnp.bfloat16
    )


def kernel(
    shape, q_in, k_in, v_in, rows_in, columns_in, far_in, out,
    q_own, q_swap, k_own, v_own, k_send, v_send, k_buf, v_buf, q_rot,
    s_even, s_odd, w_even, w_odd, row_table, near_tables, far_table,
    peak, total, fade, top, acc, o_buf,
    local_sem, swap_send, swap_recv, sent_sem, column_sem, near_sem, cross_sem, out_sem,
):
    shard, pairs, side_a, side_b, sequences, span = shape
    rows = 2 * shard
    length = pairs * rows
    s = lax.axis_index("seq")
    g = lax.axis_index("stretch")
    h = s % 2
    p = s // 2
    a = p // side_b
    b = p % side_b
    n = g // sequences
    last = BLOCKS - 1
    partner = {"seq": s + 1 - 2 * h}
    mesh_type = pl.DeviceIdType.MESH

    def pair_at(a_index, b_index):
        return a_index * side_b + b_index

    def device_at(pair, core):
        return {"seq": 2 * pair + core}

    def block_at(shift, core):
        return {"seq": 2 * p + core, "stretch": g + shift * sequences}

    a_peers = [pair_at((a + i) % side_a, b) for i in range(1, side_a)]
    b_peers = [pair_at(a, (b + j) % side_b) for j in range(1, side_b)]
    diagonal = [
        pair_at((a + i) % side_a, (b + j) % side_b)
        for i in range(1, side_a)
        for j in range(1, side_b)
    ]
    across_a, across_b = len(a_peers), len(b_peers)
    across = across_a * across_b

    def at(start, size, unit):
        return pl.ds(pl.multiple_of(start, unit), size)

    def half_columns(core):
        return at(core * shard, shard, shard)

    mine = half_columns(h)
    theirs = half_columns(1 - h)

    local = [
        (k_in, k_own, 0),
        (rows_in.at[at(p * rows + h * shard, shard, shard), :], row_table, 1),
        (v_in, v_own, 2),
        (q_in, q_own, 3),
        (columns_in.at[:, at(p * rows, rows, rows)], near_tables.at[0], 4),
        (columns_in.at[:, at(length + p * rows, rows, rows)], near_tables.at[1], 4),
        (far_in, far_table, 5),
    ]
    local = [pltpu.make_async_copy(src, dst, local_sem.at[i]) for src, dst, i in local]
    for copy in local:
        copy.start()

    barrier = pltpu.get_barrier_semaphore()

    def greet(device):
        pl.semaphore_signal(barrier, inc=1, device_id=device, device_id_type=mesh_type)

    for core in range(2):
        @pl.when(n < last)
        def _():
            greet(block_at(1, core))

        @pl.when(n > 0)
        def _():
            greet(block_at(-1, core))

        @pl.when((n == 0) | (n == last))
        def _():
            greet(partner)

        for peer in a_peers + b_peers:
            greet(device_at(peer, core))
    greet(partner)

    for copy in local[:3]:
        copy.wait()
    for head in range(KEY_VALUE_HEADS):
        columns = slice(head * HEAD_SIZE, (head + 1) * HEAD_SIZE)
        k_send[head] = turned_rows(k_own[:, columns], row_table[...])
        v_send[head] = v_own[:, columns].T

    def slot(t, d, pair):
        return (k_buf, v_buf)[t].at[pl.ds((d * pairs + pair) * 2, 2)]

    def place(d, pair, core):
        return (d * pairs + pair) * 2 + core

    k_buf[place(0, p, h)] = k_send[h]
    v_buf[place(0, p, h)] = v_send[h]
    pl.semaphore_wait(barrier, 1 + 2 * (across_a + across_b) + 4)

    def send(src, dst, sent, received, device):
        return pltpu.make_async_remote_copy(
            src_ref=src, dst_ref=dst, send_sem=sent, recv_sem=received,
            device_id=device, device_id_type=mesh_type,
        )

    def halves(count):
        return k_buf.at[pl.ds(0, count)]

    def await_slots(count, received):
        some = halves(2 * count)
        send(some, some, swap_send, received, partner).wait_recv()

    def first(t, core, device, d_to, received):
        dst = (k_buf, v_buf)[t].at[place(d_to, p, h)]
        send((k_send, v_send)[t].at[core], dst, sent_sem.at[t, 0], received, device).start()

    def message(t, d, pair, device, d_to, group, received):
        src, dst = slot(t, d, pair), slot(t, d_to, pair)
        send(src, dst, sent_sem.at[t, group], received, device).start()

    def peers(t, d):
        return [(peer, near_sem.at[t, d]) for peer in b_peers + a_peers]

    query_swap = send(
        q_own.at[:, at((1 - h) * WIDTH, WIDTH, HEAD_SIZE)], q_swap,
        swap_send, swap_recv.at[1], partner,
    )
    for t in range(2):
        for peer, received in peers(t, 0):
            for core in range(2):
                first(t, core, device_at(peer, core), 0, received)

        @pl.when(n < last)
        def _():
            for core in range(2):
                first(t, core, block_at(1, core), 1, column_sem.at[t, 1])

        first(t, 1 - h, partner, 0, swap_recv.at[0])
    local[3].wait()
    query_swap.start()

    def column(t, d):
        await_slots(1, column_sem.at[t, d])
        for peer, received in peers(t, d):
            message(t, d, p, device_at(peer, h), d, 0, received)

        if not (isinstance(d, int) and d == last):
            @pl.when(n < last)
            def _():
                message(t, d, p, block_at(1, h), d + 1, 0, column_sem.at[t, d + 1])

    def relayed(d):
        return (d == 0) | (d == n - 1)

    def pass_on(t, d):
        sources, targets = ((b_peers, a_peers), (a_peers, b_peers))[t]
        await_slots(across_a + across_b, near_sem.at[t, d])

        @pl.when(relayed(d))
        def _():
            for source in sources:
                for target in targets:
                    message(t, d, source, device_at(target, h), d, 1, cross_sem.at[t, d])

    def cross(d):
        for t in range(2):
            await_slots(across, cross_sem.at[t, d])

            @pl.when(((n < last) & (n == d)) | ((n == last - 1) & (d == 0)))
            def _():
                for pair in diagonal:
                    message(t, d, pair, block_at(1, h), d + 1, 1, cross_sem.at[t, d + 1])

    def rotate_queries(source, half):
        near, later, far = near_tables[0, :, half], near_tables[1, :, half], far_table[:, :1]
        for c in range(CLUSTER):
            x = source(c).T.astype(jnp.float32)
            for version, table in enumerate((near, later, far)):
                scaled = turned_columns(x, table).astype(jnp.float32) * SCALE
                high = scaled.astype(jnp.bfloat16)
                q_rot[version, c, :HEAD_SIZE, half] = high
                rest = scaled - high.astype(jnp.float32)
                q_rot[version, c, HEAD_SIZE:, half] = rest.astype(jnp.bfloat16)

    def scores(c, starts, version, causal, into, side):
        highest = None
        for i in range(2 * len(starts)):
            keys = k_buf[starts[i // 2] + i % 2]
            keys = jnp.concatenate([keys, keys], axis=1)
            found = jnp.dot(keys, q_rot[version, c], preferred_element_type=jnp.float32)
            if causal:
                key = i * shard + lax.broadcasted_iota(jnp.int32, found.shape, 0)
                row = b * rows + lax.broadcasted_iota(jnp.int32, found.shape, 1)
                found = jnp.where(row >= key, found, MASKED)
            into[i * shard : (i + 1) * shard, :] = found
            some = jnp.max(found.reshape(shard // 8, 8, rows), axis=0)
            highest = some if highest is None else jnp.maximum(highest, some)
        top[side] = highest

    def weigh(c, causal, source, into, side):
        new = jnp.max(top[side], axis=0, keepdims=True)
        if causal:
            new = jnp.broadcast_to(new, (8, rows))
        else:
            old = peak[c]
            new = jnp.maximum(old, new)
            fade[side] = jnp.exp2(old - new)
        peak[c] = new
        new = new[:1]
        added = None
        for start in range(0, span, 64):
            weights = jnp.exp2(source[start : start + 64, :] - new)
            some = jnp.sum(weights.reshape(8, 8, rows), axis=0)
            added = some if added is None else added + some
            into[start : start + 64, :] = weights.astype(jnp.bfloat16)
        total[c] = added if causal else total[c] * fade[side] + added

    def gather(c, starts, causal, source, side):
        product = None
        for i, start in enumerate(starts):
            values = jnp.concatenate([v_buf[start], v_buf[start + 1]], axis=1)
            some = jnp.dot(
                values, source[i * rows : (i + 1) * rows, :], preferred_element_type=jnp.float32
            )
            product = some if product is None else product + some
        acc[c] = product if causal else acc[c] * fade[side][:1] + product

    def result(c):
        where = at((h * CLUSTER + c) * HEAD_SIZE, HEAD_SIZE, HEAD_SIZE)
        return send(
            o_buf.at[c, theirs, :], out.at[:, where], out_sem.at[0], out_sem.at[1], partner
        )

    def finish(c):
        share = 1.0 / jnp.sum(total[c], axis=0, keepdims=True)
        o_buf[c] = (acc[c] * share).astype(jnp.bfloat16).T
        out[:, at((h * CLUSTER + c) * HEAD_SIZE, HEAD_SIZE, HEAD_SIZE)] = o_buf[c, mine, :]

    def in_line(d, line):
        return [place(d, line * side_b + i, 0) for i in range(side_b)]

    def attend(starts, version, causal, final):
        s_buf, w_buf = (s_even, s_odd), (w_even, w_odd)
        scores(0, starts, version, causal, s_buf[0], 0)
        for c in range(CLUSTER + 1):
            if c + 1 < CLUSTER:
                scores(c + 1, starts, version, causal, s_buf[(c + 1) % 2], (c + 1) % 2)
            if c > 0:
                gather(c - 1, starts, causal, w_buf[(c - 1) % 2], (c - 1) % 2)
                if final:
                    finish(c - 1)
                    if c > 1:
                        result(c - 2).start()
            if c < CLUSTER:
                weigh(c, causal, s_buf[c % 2], w_buf[c % 2], c % 2)
        if final:
            result(CLUSTER - 1).start()

    for copy in local[6:]:
        copy.wait()
    pltpu.make_async_copy(near_tables, near_tables, local_sem.at[4]).wait()
    rotate_queries(lambda c: q_own[:, at(h * WIDTH + c * HEAD_SIZE, HEAD_SIZE, HEAD_SIZE)], mine)
    query_swap.wait_recv()
    rotate_queries(lambda c: q_swap[:, c * HEAD_SIZE : (c + 1) * HEAD_SIZE], theirs)
    await_slots(1, swap_recv.at[0])

    for t in range(2):
        pass_on(t, 0)

        @pl.when(n > 0)
        def _():
            column(t, 1)

    attend(in_line(0, a), 0, True, False)

    many = n >= 2
    most = n == last
    square = side_a == 2 and side_b == 2

    def choose(j, *pairs):
        found = pairs[-1]
        for when, value in reversed(pairs[:-1]):
            found = jnp.where((j == when), value, found)
        return found

    def visit(j, carry):
        d = jnp.where(j < 2, 0, jnp.where((j == 2) | (j == 4), 1, 2))
        d = jnp.where((j == 3) & (n == 1), 1, d)
        d = jnp.where(((j == 5) & most) | (j == 7), last, d)
        other = (j == 1) | (j == 4) | (j > 5) | ((j == 3) & (n == 1)) | ((j == 5) & (n == 2))
        near = jnp.logical_not(other)
        if square:
            d = jnp.where(most, choose(j, (1, 0), (4, 2), (6, 3), (3, 2), (7, 2), 1), d)
            other = jnp.where(most, ((j == 1) | (j == 5)).astype(jnp.int32), other.astype(jnp.int32)) == 1
            near = (most & (j % 2 == 0)) | (jnp.logical_not(most) & near)

        for t, d_in, stage, when in (
            (0, 2, 1, many), (1, 2, 1, many), (0, last, 2, most), (1, last, 3, most)
        ):
            @pl.when((j == stage) & when)
            def _():
                column(t, d_in)

        @pl.when(near)
        def _():
            pass_on(0, d)
            pass_on(1, d)

        late = ((1, 5), (2, 7), (last, 7)) if square else ((1, 4), (2, 6), (last, 7))
        for d_in, stage, when in [(0, 1, n >= 0), (1, 2, n == 1), (2, 3, n == 2), (1, 4, n == 2)] + [
            (d_in, stage, most) for d_in, stage in late
        ]:
            @pl.when((j == stage) & when)
            def _():
                cross(d_in)

        def inner(i, inside):
            line = (a + i) % side_a
            starts = in_line(d, line)
            if square:
                pick = [
                    [place(2, p, 0), place(last, p, 0)],
                    [place(2, b_peers[0], 0), place(2, a_peers[0], 0)],
                    [place(last, b_peers[0], 0), place(last, a_peers[0], 0)],
                ]
                starts = [
                    jnp.where(most, choose(j, *zip((3, 4, 6), options), start), start)
                    for start, *options in zip(starts, *pick)
                ]

            @pl.when((d > 0) | (line < a))
            def _():
                attend(starts, jnp.minimum(d, 2), False, False)

            return inside

        ends = jnp.where(other, side_a, 1) - jnp.where(j == 2 * n + 1, 1, 0)
        begins = jnp.where(other, 1, 0)
        return lax.fori_loop(begins, ends, inner, carry)

    lax.fori_loop(1, 2 * (n + 1), visit, 0)
    line = (a + side_a - 1) % side_a
    reached = (n > 0) | (line < a)
    starts = in_line(n, line)
    if square:
        options = [place(2, diagonal[0], 0), place(last, diagonal[0], 0)]
        starts = [jnp.where(most, option, start) for option, start in zip(options, starts)]

    @pl.when(reached)
    def _():
        attend(starts, jnp.minimum(n, 2), False, True)

    @pl.when(jnp.logical_not(reached))
    def _():
        for c in range(CLUSTER + 1):
            if c < CLUSTER:
                finish(c)
            if c > 0:
                result(c - 1).start()

    query_swap.wait_send()
    for k in range(BLOCKS):
        lifted = 2 if k < last else 0
        direct = 2 * (across_a + across_b)
        counts = (
            direct + 1 + lifted + k * (direct + lifted),
            2 * across * ((2 if k > 1 else 1) + (k < last) + (k == last - 1)),
        )

        @pl.when(n == k)
        def _():
            for t in range(2):
                for group, count in enumerate(counts):
                    if count:
                        some = halves(count)
                        send(
                            some, some, sent_sem.at[t, group], swap_recv.at[0], partner
                        ).wait_send()

    whole = send(q_swap, q_swap, out_sem.at[0], out_sem.at[1], partner)
    whole.wait_send()
    whole.wait_recv()


def on_device(queries, keys, values):
    shard = queries.shape[0]
    pairs = lax.axis_size("seq") // 2
    sequences = lax.axis_size("stretch") // BLOCKS
    side_a = max(i for i in range(1, pairs + 1) if pairs % i == 0 and i * i <= pairs)
    side_b = pairs // side_a
    rows = 2 * shard
    length = pairs * rows
    span = side_b * rows
    shape = (shard, pairs, side_a, side_b, sequences, span)
    table = rotary_table(2 * length)
    far = np.broadcast_to(table[-1][:, None], (HEAD_SIZE, HEAD_SIZE))
    dma = pltpu.SemaphoreType.DMA
    bf16, f32 = jnp.bfloat16, jnp.float32
    return pl.pallas_call(
        functools.partial(kernel, shape),
        out_shape=pltpu.VMEM(queries.shape, bf16),
        in_specs=[pl.BlockSpec(memory_space=pl.ANY)] * 6,
        scratch_shapes=[
            pltpu.VMEM((shard, 2 * WIDTH), bf16),
            pltpu.VMEM((shard, WIDTH), bf16),
            pltpu.VMEM((shard, 2 * HEAD_SIZE), bf16),
            pltpu.VMEM((shard, 2 * HEAD_SIZE), bf16),
            pltpu.VMEM((2, shard, HEAD_SIZE), bf16),
            pltpu.VMEM((2, HEAD_SIZE, shard), bf16),
            pltpu.VMEM((BLOCKS * pairs * 2, shard, HEAD_SIZE), bf16),
            pltpu.VMEM((BLOCKS * pairs * 2, HEAD_SIZE, shard), bf16),
            pltpu.VMEM((3, CLUSTER, 2 * HEAD_SIZE, rows), bf16),
            pltpu.VMEM((span, rows), f32),
            pltpu.VMEM((span, rows), f32),
            pltpu.VMEM((span, rows), bf16),
            pltpu.VMEM((span, rows), bf16),
            pltpu.VMEM((shard, HEAD_SIZE), f32),
            pltpu.VMEM((2, HEAD_SIZE, rows), f32),
            pltpu.VMEM((HEAD_SIZE, HEAD_SIZE), f32),
            pltpu.VMEM((CLUSTER, 8, rows), f32),
            pltpu.VMEM((CLUSTER, 8, rows), f32),
            pltpu.VMEM((2, 8, rows), f32),
            pltpu.VMEM((2, 8, rows), f32),
            pltpu.VMEM((CLUSTER, HEAD_SIZE, rows), f32),
            pltpu.VMEM((CLUSTER, rows, HEAD_SIZE), bf16),
            dma((6,)),
            dma(()),
            dma((2,)),
            dma((2, 2)),
            dma((2, BLOCKS)),
            dma((2, BLOCKS)),
            dma((2, BLOCKS)),
            dma((2,)),
        ],
        compiler_params=pltpu.CompilerParams(
            collective_id=0, has_side_effects=True, vmem_limit_bytes=60 * 1024 * 1024
        ),
    )(
        queries, keys, values,
        jnp.asarray(table[:length]), jnp.asarray(np.ascontiguousarray(table.T)), jnp.asarray(far),
    )


def solution(mesh):
    placed = P(("stretch", "seq"), None)
    return jax.shard_map(
        on_device, mesh=mesh, in_specs=(placed,) * 3, out_specs=placed, check_vma=False
    )
```

```python
import functools
import math

import jax
import jax.numpy as jnp
import numpy as np
from jax import lax
from jax.experimental import pallas as pl
from jax.experimental.pallas import tpu as pltpu
from jax.sharding import PartitionSpec as P

QUERY_HEADS = 14
KEY_VALUE_HEADS = 2
HEAD_SIZE = 128
BLOCKS = 4
CLUSTER = QUERY_HEADS // KEY_VALUE_HEADS
WIDTH = CLUSTER * HEAD_SIZE
HALF = HEAD_SIZE // 2
SCALE = math.log2(math.e) / math.sqrt(HEAD_SIZE)
MASKED = -1e30


def rotary_table(positions):
    inverse = 10000000.0 ** (-(np.arange(HALF, dtype=np.float64) * 2.0) / HEAD_SIZE)
    angles = np.arange(positions, dtype=np.float64)[:, None] * inverse[None, :]
    return np.concatenate([np.cos(angles), np.sin(angles)], axis=1).astype(np.float32)


def turned_rows(rows, table):
    swapped = pltpu.roll(table, HALF, 1)
    low = lax.broadcasted_iota(jnp.int32, table.shape, 1) < HALF
    cosine, sine = jnp.where(low, table, swapped), jnp.where(low, -swapped, table)
    x = rows.astype(jnp.float32)
    return (x * cosine + pltpu.roll(x, HALF, 1) * sine).astype(jnp.bfloat16)


def turned_columns(columns, table):
    x, y = columns[:HALF], columns[HALF:]
    cosine, sine = table[:HALF], table[HALF:]
    return jnp.concatenate([x * cosine - y * sine, y * cosine + x * sine], axis=0).astype(
        jnp.bfloat16
    )


def kernel(
    shape, q_in, k_in, v_in, rows_in, columns_in, far_in, out,
    q_own, q_swap, k_own, v_own, k_send, v_send, k_buf, v_buf, q_rot,
    s_even, s_odd, w_even, w_odd, row_table, near_tables, far_table,
    peak, total, fade, top, acc, o_buf,
    local_sem, swap_send, swap_recv, sent_sem, column_sem, near_sem, cross_sem, out_sem,
):
    shard, pairs, side_a, side_b, sequences, span = shape
    rows = 2 * shard
    length = pairs * rows
    s = lax.axis_index("seq")
    g = lax.axis_index("stretch")
    h = s % 2
    p = s // 2
    a = p // side_b
    b = p % side_b
    n = g // sequences
    last = BLOCKS - 1
    partner = {"seq": s + 1 - 2 * h}
    mesh_type = pl.DeviceIdType.MESH

    def pair_at(a_index, b_index):
        return a_index * side_b + b_index

    def device_at(pair, core):
        return {"seq": 2 * pair + core}

    def block_at(shift, core):
        return {"seq": 2 * p + core, "stretch": g + shift * sequences}

    a_peers = [pair_at((a + i) % side_a, b) for i in range(1, side_a)]
    b_peers = [pair_at(a, (b + j) % side_b) for j in range(1, side_b)]
    diagonal = [
        pair_at((a + i) % side_a, (b + j) % side_b)
        for i in range(1, side_a)
        for j in range(1, side_b)
    ]
    across_a, across_b = len(a_peers), len(b_peers)
    across = across_a * across_b

    def at(start, size, unit):
        return pl.ds(pl.multiple_of(start, unit), size)

    def half_columns(core):
        return at(core * shard, shard, shard)

    mine = half_columns(h)
    theirs = half_columns(1 - h)

    local = [
        (k_in, k_own, 0),
        (rows_in.at[at(p * rows + h * shard, shard, shard), :], row_table, 0),
        (v_in, v_own, 0),
        (q_in, q_own, 1),
        (columns_in.at[:, at(p * rows, rows, rows)], near_tables.at[0], 2),
        (columns_in.at[:, at(length + p * rows, rows, rows)], near_tables.at[1], 2),
        (far_in, far_table, 3),
    ]
    local = [pltpu.make_async_copy(src, dst, local_sem.at[i]) for src, dst, i in local]
    for copy in local:
        copy.start()

    barrier = pltpu.get_barrier_semaphore()

    def greet(device):
        pl.semaphore_signal(barrier, inc=1, device_id=device, device_id_type=mesh_type)

    for core in range(2):
        @pl.when(n < last)
        def _():
            greet(block_at(1, core))

        @pl.when(n > 0)
        def _():
            greet(block_at(-1, core))

        @pl.when((n == 0) | (n == last))
        def _():
            greet(partner)

        for peer in a_peers + b_peers:
            greet(device_at(peer, core))
    greet(partner)

    early = q_own.at[:, pl.ds(0, 6 * HEAD_SIZE)]
    pltpu.make_async_copy(early, early, local_sem.at[0]).wait()
    for head in range(KEY_VALUE_HEADS):
        columns = slice(head * HEAD_SIZE, (head + 1) * HEAD_SIZE)
        k_send[head] = turned_rows(k_own[:, columns], row_table[...])
        v_send[head] = v_own[:, columns].T

    def slot(t, d, pair):
        return (k_buf, v_buf)[t].at[pl.ds((d * pairs + pair) * 2, 2)]

    def place(d, pair, core):
        return (d * pairs + pair) * 2 + core

    k_buf[place(0, p, h)] = k_send[h]
    v_buf[place(0, p, h)] = v_send[h]
    pl.semaphore_wait(barrier, 1 + 2 * (across_a + across_b) + 4)

    def send(src, dst, sent, received, device):
        return pltpu.make_async_remote_copy(
            src_ref=src, dst_ref=dst, send_sem=sent, recv_sem=received,
            device_id=device, device_id_type=mesh_type,
        )

    def halves(count):
        return k_buf.at[pl.ds(0, count)]

    def await_slots(count, received):
        some = halves(2 * count)
        send(some, some, swap_send, received, partner).wait_recv()

    def first(t, core, device, d_to, received):
        dst = (k_buf, v_buf)[t].at[place(d_to, p, h)]
        send((k_send, v_send)[t].at[core], dst, sent_sem.at[t, 0], received, device).start()

    def message(t, d, pair, device, d_to, group, received):
        src, dst = slot(t, d, pair), slot(t, d_to, pair)
        send(src, dst, sent_sem.at[t, group], received, device).start()

    def peers(t, d):
        return [(peer, near_sem.at[t if isinstance(d, int) and d == 0 else d + 1]) for peer in b_peers + a_peers]

    query_swap = send(
        q_own.at[:, at((1 - h) * WIDTH, WIDTH, HEAD_SIZE)], q_swap,
        swap_send, swap_recv.at[1], partner,
    )
    for t in range(2):
        for peer, received in peers(t, 0):
            for core in range(2):
                first(t, core, device_at(peer, core), 0, received)

        @pl.when(n < last)
        def _():
            for core in range(2):
                first(t, core, block_at(1, core), 1, column_sem.at[t, 0])

        first(t, 1 - h, partner, 0, swap_recv.at[0])
    local[3].wait()
    query_swap.start()

    def column(t, d):
        await_slots(1, column_sem.at[t, d - 1])
        for peer, received in peers(t, d):
            message(t, d, p, device_at(peer, h), d, 0, received)

        if not (isinstance(d, int) and d == last):
            @pl.when(n < last)
            def _():
                message(t, d, p, block_at(1, h), d + 1, 0, column_sem.at[t, d])

    def relayed(d):
        return (d == 0) | (d == n - 1)

    def pass_on(sides, d, received):
        await_slots(len(sides) * (across_a + across_b), received)

        @pl.when(relayed(d))
        def _():
            for t in sides:
                sources, targets = ((b_peers, a_peers), (a_peers, b_peers))[t]
                for source in sources:
                    for target in targets:
                        message(t, d, source, device_at(target, h), d, 1, cross_sem.at[t, d])

    def cross(d):
        for t in range(2):
            await_slots(across, cross_sem.at[t, d])

            @pl.when(((n < last) & (n == d)) | ((n == last - 1) & (d == 0)))
            def _():
                for pair in diagonal:
                    message(t, d, pair, block_at(1, h), d + 1, 1, cross_sem.at[t, d + 1])

    def rotate_queries(source, half):
        near, later, far = near_tables[0, :, half], near_tables[1, :, half], far_table[:, :1]
        for c in range(CLUSTER):
            x = source(c).T.astype(jnp.float32)
            for version, table in enumerate((near, later, far)):
                scaled = turned_columns(x, table).astype(jnp.float32) * SCALE
                high = scaled.astype(jnp.bfloat16)
                q_rot[version, c, :HEAD_SIZE, half] = high
                rest = scaled - high.astype(jnp.float32)
                q_rot[version, c, HEAD_SIZE:, half] = rest.astype(jnp.bfloat16)

    def scores(c, starts, version, causal, into, side):
        highest = None
        for i in range(2 * len(starts)):
            keys = k_buf[starts[i // 2] + i % 2]
            keys = jnp.concatenate([keys, keys], axis=1)
            found = jnp.dot(keys, q_rot[version, c], preferred_element_type=jnp.float32)
            if causal:
                key = i * shard + lax.broadcasted_iota(jnp.int32, found.shape, 0)
                row = b * rows + lax.broadcasted_iota(jnp.int32, found.shape, 1)
                found = jnp.where(row >= key, found, MASKED)
            into[i * shard : (i + 1) * shard, :] = found
            some = jnp.max(found.reshape(shard // 8, 8, rows), axis=0)
            highest = some if highest is None else jnp.maximum(highest, some)
        top[side] = highest

    def weigh(c, causal, source, into, side):
        new = jnp.max(top[side], axis=0, keepdims=True)
        if causal:
            new = jnp.broadcast_to(new, (8, rows))
        else:
            old = peak[c]
            new = jnp.maximum(old, new)
            fade[side] = jnp.exp2(old - new)
        peak[c] = new
        new = new[:1]
        added = None
        for start in range(0, span, 64):
            weights = jnp.exp2(source[start : start + 64, :] - new)
            some = jnp.sum(weights.reshape(8, 8, rows), axis=0)
            added = some if added is None else added + some
            into[start : start + 64, :] = weights.astype(jnp.bfloat16)
        total[c] = added if causal else total[c] * fade[side] + added

    def gather(c, starts, causal, source, side):
        product = None
        for i, start in enumerate(starts):
            values = jnp.concatenate([v_buf[start], v_buf[start + 1]], axis=1)
            some = jnp.dot(
                values, source[i * rows : (i + 1) * rows, :], preferred_element_type=jnp.float32
            )
            product = some if product is None else product + some
        acc[c] = product if causal else acc[c] * fade[side][:1] + product

    def result(c):
        where = at((h * CLUSTER + c) * HEAD_SIZE, HEAD_SIZE, HEAD_SIZE)
        return send(
            o_buf.at[c, theirs, :], out.at[:, where], out_sem.at[0], out_sem.at[1], partner
        )

    def finish(c):
        share = 1.0 / jnp.sum(total[c], axis=0, keepdims=True)
        o_buf[c] = (acc[c] * share).astype(jnp.bfloat16).T
        out[:, at((h * CLUSTER + c) * HEAD_SIZE, HEAD_SIZE, HEAD_SIZE)] = o_buf[c, mine, :]

    def in_line(d, line):
        return [place(d, line * side_b + i, 0) for i in range(side_b)]

    def attend(starts, version, causal, final):
        s_buf, w_buf = (s_even, s_odd), (w_even, w_odd)
        scores(0, starts, version, causal, s_buf[0], 0)
        for c in range(CLUSTER + 1):
            if c + 1 < CLUSTER:
                scores(c + 1, starts, version, causal, s_buf[(c + 1) % 2], (c + 1) % 2)
            if c > 0:
                gather(c - 1, starts, causal, w_buf[(c - 1) % 2], (c - 1) % 2)
                if final:
                    finish(c - 1)
                    if c > 1:
                        result(c - 2).start()
            if c < CLUSTER:
                weigh(c, causal, s_buf[c % 2], w_buf[c % 2], c % 2)
        if final:
            result(CLUSTER - 1).start()

    for copy in local[6:]:
        copy.wait()
    pltpu.make_async_copy(near_tables, near_tables, local_sem.at[2]).wait()
    rotate_queries(lambda c: q_own[:, at(h * WIDTH + c * HEAD_SIZE, HEAD_SIZE, HEAD_SIZE)], mine)
    query_swap.wait_recv()
    rotate_queries(lambda c: q_swap[:, c * HEAD_SIZE : (c + 1) * HEAD_SIZE], theirs)
    await_slots(1, swap_recv.at[0])

    for t in range(2):
        pass_on((t,), 0, near_sem.at[t])

        @pl.when(n > 0)
        def _():
            column(t, 1)

    attend(in_line(0, a), 0, True, False)

    many = n >= 2
    most = n == last
    square = side_a == 2 and side_b == 2

    def choose(j, *pairs):
        found = pairs[-1]
        for when, value in reversed(pairs[:-1]):
            found = jnp.where((j == when), value, found)
        return found

    def visit(j, carry):
        d = jnp.where(j < 2, 0, jnp.where((j == 2) | (j == 4), 1, 2))
        d = jnp.where((j == 3) & (n == 1), 1, d)
        d = jnp.where(((j == 5) & most) | (j == 7), last, d)
        other = (j == 1) | (j == 4) | (j > 5) | ((j == 3) & (n == 1)) | ((j == 5) & (n == 2))
        near = jnp.logical_not(other)
        if square:
            d = jnp.where(most, choose(j, (1, 0), (4, 2), (6, 3), (3, 2), (7, 2), 1), d)
            other = jnp.where(most, ((j == 1) | (j == 5)).astype(jnp.int32), other.astype(jnp.int32)) == 1
            near = (most & (j % 2 == 0)) | (jnp.logical_not(most) & near)

        for t, d_in, stage, when in (
            (0, 2, 1, many), (1, 2, 1, many), (0, last, 2, most), (1, last, 3, most)
        ):
            @pl.when((j == stage) & when)
            def _():
                column(t, d_in)

        late = ((1, 5), (2, 7), (last, 7)) if square else ((1, 4), (2, 6), (last, 7))
        for d_in, stage, when in [(0, 1, n >= 0), (1, 2, n == 1), (2, 3, n == 2), (1, 4, n == 2)] + [
            (d_in, stage, most) for d_in, stage in late
        ]:
            @pl.when((j == stage) & when)
            def _():
                cross(d_in)

        @pl.when(near)
        def _():
            pass_on((0, 1), d, near_sem.at[d + 1])

        def inner(i, inside):
            line = (a + i) % side_a
            starts = in_line(d, line)
            if square:
                pick = [
                    [place(2, p, 0), place(last, p, 0)],
                    [place(2, b_peers[0], 0), place(2, a_peers[0], 0)],
                    [place(last, b_peers[0], 0), place(last, a_peers[0], 0)],
                ]
                starts = [
                    jnp.where(most, choose(j, *zip((3, 4, 6), options), start), start)
                    for start, *options in zip(starts, *pick)
                ]

            @pl.when((d > 0) | (line < a))
            def _():
                attend(starts, jnp.minimum(d, 2), False, False)

            return inside

        ends = jnp.where(other, side_a, 1) - jnp.where(j == 2 * n + 1, 1, 0)
        begins = jnp.where(other, 1, 0)
        return lax.fori_loop(begins, ends, inner, carry)

    lax.fori_loop(1, 2 * (n + 1), visit, 0)
    line = (a + side_a - 1) % side_a
    reached = (n > 0) | (line < a)
    starts = in_line(n, line)
    if square:
        options = [place(2, diagonal[0], 0), place(last, diagonal[0], 0)]
        starts = [jnp.where(most, option, start) for option, start in zip(options, starts)]

    @pl.when(reached)
    def _():
        attend(starts, jnp.minimum(n, 2), False, True)

    @pl.when(jnp.logical_not(reached))
    def _():
        for c in range(CLUSTER + 1):
            if c < CLUSTER:
                finish(c)
            if c > 0:
                result(c - 1).start()

    query_swap.wait_send()
    for k in range(BLOCKS):
        lifted = 2 if k < last else 0
        direct = 2 * (across_a + across_b)
        counts = (
            direct + 1 + lifted + k * (direct + lifted),
            2 * across * ((2 if k > 1 else 1) + (k < last) + (k == last - 1)),
        )

        @pl.when(n == k)
        def _():
            for t in range(2):
                for group, count in enumerate(counts):
                    if count:
                        some = halves(count)
                        send(
                            some, some, sent_sem.at[t, group], swap_recv.at[0], partner
                        ).wait_send()

    whole = send(q_swap, q_swap, out_sem.at[0], out_sem.at[1], partner)
    whole.wait_send()
    whole.wait_recv()


def on_device(queries, keys, values):
    shard = queries.shape[0]
    pairs = lax.axis_size("seq") // 2
    sequences = lax.axis_size("stretch") // BLOCKS
    side_a = max(i for i in range(1, pairs + 1) if pairs % i == 0 and i * i <= pairs)
    side_b = pairs // side_a
    rows = 2 * shard
    length = pairs * rows
    span = side_b * rows
    shape = (shard, pairs, side_a, side_b, sequences, span)
    table = rotary_table(2 * length)
    far = np.broadcast_to(table[-1][:, None], (HEAD_SIZE, HEAD_SIZE))
    dma = pltpu.SemaphoreType.DMA
    bf16, f32 = jnp.bfloat16, jnp.float32
    return pl.pallas_call(
        functools.partial(kernel, shape),
        out_shape=pltpu.VMEM(queries.shape, bf16),
        in_specs=[pl.BlockSpec(memory_space=pl.ANY)] * 6,
        scratch_shapes=[
            pltpu.VMEM((shard, 2 * WIDTH), bf16),
            pltpu.VMEM((shard, WIDTH), bf16),
            pltpu.VMEM((shard, 2 * HEAD_SIZE), bf16),
            pltpu.VMEM((shard, 2 * HEAD_SIZE), bf16),
            pltpu.VMEM((2, shard, HEAD_SIZE), bf16),
            pltpu.VMEM((2, HEAD_SIZE, shard), bf16),
            pltpu.VMEM((BLOCKS * pairs * 2, shard, HEAD_SIZE), bf16),
            pltpu.VMEM((BLOCKS * pairs * 2, HEAD_SIZE, shard), bf16),
            pltpu.VMEM((3, CLUSTER, 2 * HEAD_SIZE, rows), bf16),
            pltpu.VMEM((span, rows), f32),
            pltpu.VMEM((span, rows), f32),
            pltpu.VMEM((span, rows), bf16),
            pltpu.VMEM((span, rows), bf16),
            pltpu.VMEM((shard, HEAD_SIZE), f32),
            pltpu.VMEM((2, HEAD_SIZE, rows), f32),
            pltpu.VMEM((HEAD_SIZE, HEAD_SIZE), f32),
            pltpu.VMEM((CLUSTER, 8, rows), f32),
            pltpu.VMEM((CLUSTER, 8, rows), f32),
            pltpu.VMEM((2, 8, rows), f32),
            pltpu.VMEM((2, 8, rows), f32),
            pltpu.VMEM((CLUSTER, HEAD_SIZE, rows), f32),
            pltpu.VMEM((CLUSTER, rows, HEAD_SIZE), bf16),
            dma((4,)),
            dma(()),
            dma((2,)),
            dma((2, 2)),
            dma((2, BLOCKS - 1)),
            dma((BLOCKS + 1,)),
            dma((2, BLOCKS)),
            dma((2,)),
        ],
        compiler_params=pltpu.CompilerParams(
            collective_id=0, has_side_effects=True, vmem_limit_bytes=60 * 1024 * 1024
        ),
    )(
        queries, keys, values,
        jnp.asarray(table[:length]), jnp.asarray(np.ascontiguousarray(table.T)), jnp.asarray(far),
    )


def solution(mesh):
    placed = P(("stretch", "seq"), None)
    return jax.shard_map(
        on_device, mesh=mesh, in_specs=(placed,) * 3, out_specs=placed, check_vma=False
    )
```

```python
import functools
import math

import jax
import jax.numpy as jnp
import numpy as np
from jax import lax
from jax.experimental import pallas as pl
from jax.experimental.pallas import tpu as pltpu
from jax.sharding import PartitionSpec as P

QUERY_HEADS = 14
KEY_VALUE_HEADS = 2
HEAD_SIZE = 128
BLOCKS = 4
CLUSTER = QUERY_HEADS // KEY_VALUE_HEADS
WIDTH = CLUSTER * HEAD_SIZE
HALF = HEAD_SIZE // 2
SCALE = math.log2(math.e) / math.sqrt(HEAD_SIZE)
MASKED = -1e30


def rotary_table(positions):
    inverse = 10000000.0 ** (-(np.arange(HALF, dtype=np.float64) * 2.0) / HEAD_SIZE)
    angles = np.arange(positions, dtype=np.float64)[:, None] * inverse[None, :]
    return np.concatenate([np.cos(angles), np.sin(angles)], axis=1).astype(np.float32)


def turned_rows(rows, table):
    swapped = pltpu.roll(table, HALF, 1)
    low = lax.broadcasted_iota(jnp.int32, table.shape, 1) < HALF
    cosine, sine = jnp.where(low, table, swapped), jnp.where(low, -swapped, table)
    x = rows.astype(jnp.float32)
    return (x * cosine + pltpu.roll(x, HALF, 1) * sine).astype(jnp.bfloat16)


def turned_columns(columns, table):
    x, y = columns[:HALF], columns[HALF:]
    cosine, sine = table[:HALF], table[HALF:]
    return jnp.concatenate([x * cosine - y * sine, y * cosine + x * sine], axis=0).astype(
        jnp.bfloat16
    )


def kernel(
    shape, q_in, k_in, v_in, rows_in, columns_in, far_in, out,
    q_own, q_swap, k_own, v_own, k_send, v_send, k_buf, v_buf, q_rot,
    s_even, s_odd, w_even, w_odd, row_table, near_tables, far_table,
    peak, total, fade, top, acc, o_buf,
    local_sem, swap_send, swap_recv, sent_sem, column_sem, near_sem, cross_sem, out_sem,
):
    shard, pairs, side_a, side_b, sequences, span = shape
    rows = 2 * shard
    length = pairs * rows
    s = lax.axis_index("seq")
    g = lax.axis_index("stretch")
    h = s % 2
    p = s // 2
    a = p // side_b
    b = p % side_b
    n = g // sequences
    last = BLOCKS - 1
    partner = {"seq": s + 1 - 2 * h}
    mesh_type = pl.DeviceIdType.MESH

    def pair_at(a_index, b_index):
        return a_index * side_b + b_index

    def device_at(pair, core):
        return {"seq": 2 * pair + core}

    def block_at(shift, core):
        return {"seq": 2 * p + core, "stretch": g + shift * sequences}

    a_peers = [pair_at((a + i) % side_a, b) for i in range(1, side_a)]
    b_peers = [pair_at(a, (b + j) % side_b) for j in range(1, side_b)]
    diagonal = [
        pair_at((a + i) % side_a, (b + j) % side_b)
        for i in range(1, side_a)
        for j in range(1, side_b)
    ]
    across_a, across_b = len(a_peers), len(b_peers)
    across = across_a * across_b

    def at(start, size, unit):
        return pl.ds(pl.multiple_of(start, unit), size)

    def half_columns(core):
        return at(core * shard, shard, shard)

    mine = half_columns(h)
    theirs = half_columns(1 - h)

    local = [
        (k_in, k_own, 0),
        (rows_in.at[at(p * rows + h * shard, shard, shard), :], row_table, 0),
        (v_in, v_own, 0),
        (q_in, q_own, 1),
        (columns_in.at[:, at(p * rows, rows, rows)], near_tables.at[0], 2),
        (columns_in.at[:, at(length + p * rows, rows, rows)], near_tables.at[1], 2),
        (far_in, far_table, 3),
    ]
    local = [pltpu.make_async_copy(src, dst, local_sem.at[i]) for src, dst, i in local]
    for copy in local:
        copy.start()

    barrier = pltpu.get_barrier_semaphore()

    def greet(device):
        pl.semaphore_signal(barrier, inc=1, device_id=device, device_id_type=mesh_type)

    for core in range(2):
        @pl.when(n < last)
        def _():
            greet(block_at(1, core))

        @pl.when(n > 0)
        def _():
            greet(block_at(-1, core))

        @pl.when((n == 0) | (n == last))
        def _():
            greet(partner)

        for peer in a_peers + b_peers:
            greet(device_at(peer, core))
    greet(partner)

    early = q_own.at[:, pl.ds(0, 6 * HEAD_SIZE)]
    pltpu.make_async_copy(early, early, local_sem.at[0]).wait()
    for head in range(KEY_VALUE_HEADS):
        columns = slice(head * HEAD_SIZE, (head + 1) * HEAD_SIZE)
        k_send[head] = turned_rows(k_own[:, columns], row_table[...])
        v_send[head] = v_own[:, columns].T

    def slot(t, d, pair):
        return (k_buf, v_buf)[t].at[pl.ds((d * pairs + pair) * 2, 2)]

    def place(d, pair, core):
        return (d * pairs + pair) * 2 + core

    k_buf[place(0, p, h)] = k_send[h]
    v_buf[place(0, p, h)] = v_send[h]
    pl.semaphore_wait(barrier, 1 + 2 * (across_a + across_b) + 4)

    def send(src, dst, sent, received, device):
        return pltpu.make_async_remote_copy(
            src_ref=src, dst_ref=dst, send_sem=sent, recv_sem=received,
            device_id=device, device_id_type=mesh_type,
        )

    def halves(count):
        return k_buf.at[pl.ds(0, count)]

    def await_slots(count, received):
        some = halves(2 * count)
        send(some, some, swap_send, received, partner).wait_recv()

    def first(t, core, device, d_to, received):
        dst = (k_buf, v_buf)[t].at[place(d_to, p, h)]
        send((k_send, v_send)[t].at[core], dst, sent_sem.at[t, 0], received, device).start()

    def message(t, d, pair, device, d_to, group, received):
        src, dst = slot(t, d, pair), slot(t, d_to, pair)
        send(src, dst, sent_sem.at[t, group], received, device).start()

    def peers(t, d):
        return [(peer, near_sem.at[t if isinstance(d, int) and d == 0 else d + 1]) for peer in b_peers + a_peers]

    query_swap = send(
        q_own.at[:, at((1 - h) * WIDTH, WIDTH, HEAD_SIZE)], q_swap,
        swap_send, swap_recv.at[1], partner,
    )
    for t in range(2):
        for peer, received in peers(t, 0):
            for core in range(2):
                first(t, core, device_at(peer, core), 0, received)

        @pl.when(n < last)
        def _():
            for core in range(2):
                first(t, core, block_at(1, core), 1, column_sem.at[t, 0])

        first(t, 1 - h, partner, 0, swap_recv.at[0])
    local[3].wait()
    query_swap.start()

    def column(t, d):
        await_slots(1, column_sem.at[t, d - 1])
        for peer, received in peers(t, d):
            message(t, d, p, device_at(peer, h), d, 0, received)

        if not (isinstance(d, int) and d == last):
            @pl.when(n < last)
            def _():
                message(t, d, p, block_at(1, h), d + 1, 0, column_sem.at[t, d])

    def relayed(d):
        return (d == 0) | (d == n - 1)

    def pass_on(sides, d, received):
        await_slots(len(sides) * (across_a + across_b), received)

        @pl.when(relayed(d))
        def _():
            for t in sides:
                sources, targets = ((b_peers, a_peers), (a_peers, b_peers))[t]
                for source in sources:
                    for target in targets:
                        message(t, d, source, device_at(target, h), d, 1, cross_sem.at[t, d])

    def cross(d):
        for t in range(2):
            await_slots(across, cross_sem.at[t, d])

            @pl.when(((n < last) & (n == d)) | ((n == last - 1) & (d == 0)))
            def _():
                for pair in diagonal:
                    message(t, d, pair, block_at(1, h), d + 1, 1, cross_sem.at[t, d + 1])

    def rotate_queries(source, half):
        near, later, far = near_tables[0, :, half], near_tables[1, :, half], far_table[:, :1]
        for c in range(CLUSTER):
            x = source(c).T.astype(jnp.float32)
            for version, table in enumerate((near, later, far)):
                scaled = turned_columns(x, table).astype(jnp.float32) * SCALE
                high = scaled.astype(jnp.bfloat16)
                q_rot[version, c, :HEAD_SIZE, half] = high
                rest = scaled - high.astype(jnp.float32)
                q_rot[version, c, HEAD_SIZE:, half] = rest.astype(jnp.bfloat16)

    def scores(c, starts, version, causal, into, side):
        highest = None
        for i in range(2 * len(starts)):
            keys = k_buf[starts[i // 2] + i % 2]
            keys = jnp.concatenate([keys, keys], axis=1)
            found = jnp.dot(keys, q_rot[version, c], preferred_element_type=jnp.float32)
            if causal:
                key = i * shard + lax.broadcasted_iota(jnp.int32, found.shape, 0)
                row = b * rows + lax.broadcasted_iota(jnp.int32, found.shape, 1)
                found = jnp.where(row >= key, found, MASKED)
            into[i * shard : (i + 1) * shard, :] = found
            some = jnp.max(found.reshape(shard // 8, 8, rows), axis=0)
            highest = some if highest is None else jnp.maximum(highest, some)
        top[side] = highest

    def weigh(c, causal, source, into, side):
        new = jnp.max(top[side], axis=0, keepdims=True)
        if causal:
            new = jnp.broadcast_to(new, (8, rows))
        else:
            old = peak[c]
            new = jnp.maximum(old, new)
            fade[side] = jnp.exp2(old - new)
        peak[c] = new
        new = new[:1]
        added = None
        for start in range(0, span, 64):
            weights = jnp.exp2(source[start : start + 64, :] - new)
            some = jnp.sum(weights.reshape(8, 8, rows), axis=0)
            added = some if added is None else added + some
            into[start : start + 64, :] = weights.astype(jnp.bfloat16)
        total[c] = added if causal else total[c] * fade[side] + added

    def gather(c, starts, causal, source, side):
        product = None
        for i, start in enumerate(starts):
            values = jnp.concatenate([v_buf[start], v_buf[start + 1]], axis=1)
            some = jnp.dot(
                values, source[i * rows : (i + 1) * rows, :], preferred_element_type=jnp.float32
            )
            product = some if product is None else product + some
        for i in range(0, HEAD_SIZE, 32):
            some = product[i : i + 32]
            acc[c, i : i + 32, :] = (
                some if causal else acc[c, i : i + 32, :] * fade[side][:1] + some
            )

    def result(c):
        where = at((h * CLUSTER + c) * HEAD_SIZE, HEAD_SIZE, HEAD_SIZE)
        return send(
            o_buf.at[c, theirs, :], out.at[:, where], out_sem.at[0], out_sem.at[1], partner
        )

    def finish(c):
        share = 1.0 / jnp.sum(total[c], axis=0, keepdims=True)
        o_buf[c] = (acc[c] * share).astype(jnp.bfloat16).T
        out[:, at((h * CLUSTER + c) * HEAD_SIZE, HEAD_SIZE, HEAD_SIZE)] = o_buf[c, mine, :]

    def in_line(d, line):
        return [place(d, line * side_b + i, 0) for i in range(side_b)]

    def attend(starts, version, causal, final):
        s_buf, w_buf = (s_even, s_odd), (w_even, w_odd)
        scores(0, starts, version, causal, s_buf[0], 0)
        for c in range(CLUSTER + 1):
            if c + 1 < CLUSTER:
                scores(c + 1, starts, version, causal, s_buf[(c + 1) % 2], (c + 1) % 2)
            if c > 0:
                gather(c - 1, starts, causal, w_buf[(c - 1) % 2], (c - 1) % 2)
                if final:
                    finish(c - 1)
                    if c > 1:
                        result(c - 2).start()
            if c < CLUSTER:
                weigh(c, causal, s_buf[c % 2], w_buf[c % 2], c % 2)
        if final:
            result(CLUSTER - 1).start()

    for copy in local[6:]:
        copy.wait()
    pltpu.make_async_copy(near_tables, near_tables, local_sem.at[2]).wait()
    rotate_queries(lambda c: q_own[:, at(h * WIDTH + c * HEAD_SIZE, HEAD_SIZE, HEAD_SIZE)], mine)
    query_swap.wait_recv()
    rotate_queries(lambda c: q_swap[:, c * HEAD_SIZE : (c + 1) * HEAD_SIZE], theirs)
    await_slots(1, swap_recv.at[0])

    for t in range(2):
        pass_on((t,), 0, near_sem.at[t])

        @pl.when(n > 0)
        def _():
            column(t, 1)

    attend(in_line(0, a), 0, True, False)

    many = n >= 2
    most = n == last
    square = side_a == 2 and side_b == 2

    def choose(j, *pairs):
        found = pairs[-1]
        for when, value in reversed(pairs[:-1]):
            found = jnp.where((j == when), value, found)
        return found

    def visit(j, carry):
        d = jnp.where(j < 2, 0, jnp.where((j == 2) | (j == 4), 1, 2))
        d = jnp.where((j == 3) & (n == 1), 1, d)
        d = jnp.where(((j == 5) & most) | (j == 7), last, d)
        other = (j == 1) | (j == 4) | (j > 5) | ((j == 3) & (n == 1)) | ((j == 5) & (n == 2))
        near = jnp.logical_not(other)
        if square:
            d = jnp.where(most, choose(j, (1, 0), (4, 2), (6, 3), (3, 2), (7, 2), 1), d)
            other = jnp.where(most, ((j == 1) | (j == 5)).astype(jnp.int32), other.astype(jnp.int32)) == 1
            near = (most & (j % 2 == 0)) | (jnp.logical_not(most) & near)

        for t, d_in, stage, when in (
            (0, 2, 1, many), (1, 2, 1, many), (0, last, 2, most), (1, last, 3, most)
        ):
            @pl.when((j == stage) & when)
            def _():
                column(t, d_in)

        late = ((1, 5), (2, 7), (last, 7)) if square else ((1, 4), (2, 6), (last, 7))
        for d_in, stage, when in [(0, 1, n >= 0), (1, 2, n == 1), (2, 3, n == 2), (1, 4, n == 2)] + [
            (d_in, stage, most) for d_in, stage in late
        ]:
            @pl.when((j == stage) & when)
            def _():
                cross(d_in)

        @pl.when(near)
        def _():
            pass_on((0, 1), d, near_sem.at[d + 1])

        def inner(i, inside):
            line = (a + i) % side_a
            starts = in_line(d, line)
            if square:
                pick = [
                    [place(2, p, 0), place(last, p, 0)],
                    [place(2, b_peers[0], 0), place(2, a_peers[0], 0)],
                    [place(last, b_peers[0], 0), place(last, a_peers[0], 0)],
                ]
                starts = [
                    jnp.where(most, choose(j, *zip((3, 4, 6), options), start), start)
                    for start, *options in zip(starts, *pick)
                ]

            @pl.when((d > 0) | (line < a))
            def _():
                attend(starts, jnp.minimum(d, 2), False, False)

            return inside

        ends = jnp.where(other, side_a, 1) - jnp.where(j == 2 * n + 1, 1, 0)
        begins = jnp.where(other, 1, 0)
        return lax.fori_loop(begins, ends, inner, carry)

    lax.fori_loop(1, 2 * (n + 1), visit, 0)
    line = (a + side_a - 1) % side_a
    reached = (n > 0) | (line < a)
    starts = in_line(n, line)
    if square:
        options = [place(2, diagonal[0], 0), place(last, diagonal[0], 0)]
        starts = [jnp.where(most, option, start) for option, start in zip(options, starts)]

    @pl.when(reached)
    def _():
        attend(starts, jnp.minimum(n, 2), False, True)

    @pl.when(jnp.logical_not(reached))
    def _():
        for c in range(CLUSTER + 1):
            if c < CLUSTER:
                finish(c)
            if c > 0:
                result(c - 1).start()

    query_swap.wait_send()
    for k in range(BLOCKS):
        lifted = 2 if k < last else 0
        direct = 2 * (across_a + across_b)
        counts = (
            direct + 1 + lifted + k * (direct + lifted),
            2 * across * ((2 if k > 1 else 1) + (k < last) + (k == last - 1)),
        )

        @pl.when(n == k)
        def _():
            for t in range(2):
                for group, count in enumerate(counts):
                    if count:
                        some = halves(count)
                        send(
                            some, some, sent_sem.at[t, group], swap_recv.at[0], partner
                        ).wait_send()

    whole = send(q_swap, q_swap, out_sem.at[0], out_sem.at[1], partner)
    whole.wait_send()
    whole.wait_recv()


def on_device(queries, keys, values):
    shard = queries.shape[0]
    pairs = lax.axis_size("seq") // 2
    sequences = lax.axis_size("stretch") // BLOCKS
    side_a = max(i for i in range(1, pairs + 1) if pairs % i == 0 and i * i <= pairs)
    side_b = pairs // side_a
    rows = 2 * shard
    length = pairs * rows
    span = side_b * rows
    shape = (shard, pairs, side_a, side_b, sequences, span)
    table = rotary_table(2 * length)
    far = np.broadcast_to(table[-1][:, None], (HEAD_SIZE, HEAD_SIZE))
    dma = pltpu.SemaphoreType.DMA
    bf16, f32 = jnp.bfloat16, jnp.float32
    return pl.pallas_call(
        functools.partial(kernel, shape),
        out_shape=pltpu.VMEM(queries.shape, bf16),
        in_specs=[pl.BlockSpec(memory_space=pl.ANY)] * 6,
        scratch_shapes=[
            pltpu.VMEM((shard, 2 * WIDTH), bf16),
            pltpu.VMEM((shard, WIDTH), bf16),
            pltpu.VMEM((shard, 2 * HEAD_SIZE), bf16),
            pltpu.VMEM((shard, 2 * HEAD_SIZE), bf16),
            pltpu.VMEM((2, shard, HEAD_SIZE), bf16),
            pltpu.VMEM((2, HEAD_SIZE, shard), bf16),
            pltpu.VMEM((BLOCKS * pairs * 2, shard, HEAD_SIZE), bf16),
            pltpu.VMEM((BLOCKS * pairs * 2, HEAD_SIZE, shard), bf16),
            pltpu.VMEM((3, CLUSTER, 2 * HEAD_SIZE, rows), bf16),
            pltpu.VMEM((span, rows), f32),
            pltpu.VMEM((span, rows), f32),
            pltpu.VMEM((span, rows), bf16),
            pltpu.VMEM((span, rows), bf16),
            pltpu.VMEM((shard, HEAD_SIZE), f32),
            pltpu.VMEM((2, HEAD_SIZE, rows), f32),
            pltpu.VMEM((HEAD_SIZE, HEAD_SIZE), f32),
            pltpu.VMEM((CLUSTER, 8, rows), f32),
            pltpu.VMEM((CLUSTER, 8, rows), f32),
            pltpu.VMEM((2, 8, rows), f32),
            pltpu.VMEM((2, 8, rows), f32),
            pltpu.VMEM((CLUSTER, HEAD_SIZE, rows), f32),
            pltpu.VMEM((CLUSTER, rows, HEAD_SIZE), bf16),
            dma((4,)),
            dma(()),
            dma((2,)),
            dma((2, 2)),
            dma((2, BLOCKS - 1)),
            dma((BLOCKS + 1,)),
            dma((2, BLOCKS)),
            dma((2,)),
        ],
        compiler_params=pltpu.CompilerParams(
            collective_id=0, has_side_effects=True, vmem_limit_bytes=60 * 1024 * 1024
        ),
    )(
        queries, keys, values,
        jnp.asarray(table[:length]), jnp.asarray(np.ascontiguousarray(table.T)), jnp.asarray(far),
    )


def solution(mesh):
    placed = P(("stretch", "seq"), None)
    return jax.shard_map(
        on_device, mesh=mesh, in_specs=(placed,) * 3, out_specs=placed, check_vma=False
    )
```
